32 devices in a mesh: first: 8 (over z, core), second: 4 (over y, x).
Axes of the slice: x: 2, y: 2, z: 4, core: 2. Of those that a mesh axis runs over, the one named last changes fastest.
Arguments:
- pair_rows: bfloat16 [96, 96, 128], P('first', 'second'), may hold values from -6 to 6
- in_gain: float32 [128], replicated, may hold values from 0.25 to 1.75
- left_weight: bfloat16 [128, 128], replicated, may hold values from -0.5 to 0.5
- right_weight: bfloat16 [128, 128], replicated, may hold values from -0.5 to 0.5
- mid_gain: float32 [128], replicated, may hold values from 0.25 to 1.75
- out_weight: bfloat16 [128, 128], replicated, may hold values from -0.5 to 0.5
- out_gate: bfloat16 [128, 128], replicated, may hold values from -0.5 to 0.5
Outputs:
- triangle_out: bfloat16 [96, 96, 128], P('first', 'second')
The draws below stay inside these ranges and needn't reach their ends.
All inputs are finite; a program needn't handle non-finite values.
Results may differ from the reference program's by a relative error of at most 0.012.
Values may be sent and summed in bfloat16 or wider, within the bound.
A program may use at most 64 MiB of HBM per device.

```python
import jax
import jax.numpy as jnp
from jax import lax

RESIDUES = 96
PAIR_WIDTH = 128
MIX_WIDTH = 128


def steps_of(stream_key, dims, cuts, smallest, top_value):
    def one(position, shards_of):
        draws = jax.random.uniform(jax.random.fold_in(jax.random.fold_in(stream_key, 6), position), (shards_of,), jnp.float32, smallest / len(cuts), top_value / len(cuts))
        return jnp.repeat(jnp.exp(draws), dims[position] // shards_of).reshape((-1,) + (1,) * (len(dims) - position - 1))

    level = one(*cuts[0])
    for cut in cuts[1:]:
        level = level * one(*cut)
    return level


def gaussian(stream_key, dims, spread, limit, cuts=(), held_as=jnp.bfloat16):
    values = spread * jax.random.normal(stream_key, dims, jnp.float32)
    if cuts:
        values = values * steps_of(stream_key, dims, cuts, -0.22, 0.18)
    return jnp.clip(values, -limit, limit).astype(held_as)


def setup_inputs(seed: int = 0) -> dict:
    key_list = jax.random.split(jax.random.key(seed), 8)
    pair_rows = gaussian(key_list[0], (RESIDUES, RESIDUES, PAIR_WIDTH), 1.0, 6.0, ((0, 8), (1, 4)))
    in_gain = jnp.clip(1.0 + 0.15 * jax.random.normal(key_list[1], (PAIR_WIDTH,), jnp.float32), 0.25, 1.75)
    left_weight = gaussian(key_list[2], (PAIR_WIDTH, MIX_WIDTH), PAIR_WIDTH ** -0.5, 0.5)
    right_weight = gaussian(key_list[3], (PAIR_WIDTH, MIX_WIDTH), PAIR_WIDTH ** -0.5, 0.5)
    mid_gain = jnp.clip(1.0 + 0.15 * jax.random.normal(key_list[4], (MIX_WIDTH,), jnp.float32), 0.25, 1.75)
    out_weight = gaussian(key_list[5], (MIX_WIDTH, PAIR_WIDTH), MIX_WIDTH ** -0.5, 0.5)
    out_gate = gaussian(key_list[6], (PAIR_WIDTH, PAIR_WIDTH), PAIR_WIDTH ** -0.5, 0.5)
    return {"pair_rows": pair_rows, "in_gain": in_gain, "left_weight": left_weight, "right_weight": right_weight, "mid_gain": mid_gain, "out_weight": out_weight, "out_gate": out_gate}


def norm_channels(values, channel_gain):
    centred = values - lax.optimization_barrier(jnp.mean(values, axis=-1, keepdims=True))
    return centred * lax.rsqrt(lax.optimization_barrier(jnp.mean(centred * centred, axis=-1, keepdims=True)) + 1e-05) * channel_gain

def project_pair(pair_in, in_gain, left_weight, right_weight):
    ready = norm_channels(pair_in.astype(jnp.float32), in_gain).astype(jnp.bfloat16)
    ready = lax.optimization_barrier(ready)
    left = jnp.einsum('ijc,cd->ijd', ready.astype(jnp.float32), left_weight.astype(jnp.float32))
    right = jnp.einsum('ijc,cd->ijd', ready.astype(jnp.float32), right_weight.astype(jnp.float32))
    return (ready, left.astype(jnp.bfloat16), right.astype(jnp.bfloat16))

def to_pair(mixed, ready, mid_gain, out_weight, out_gate):
    scaled = norm_channels(mixed.astype(jnp.float32), mid_gain).astype(jnp.bfloat16)
    scaled = lax.optimization_barrier(scaled)
    gate = jax.nn.sigmoid(jnp.einsum('ijc,cd->ijd', ready.astype(jnp.float32), out_gate.astype(jnp.float32)))
    return (jnp.einsum('ijd,dc->ijc', scaled.astype(jnp.float32), out_weight.astype(jnp.float32)) * gate).astype(jnp.bfloat16)

def reference(pair_rows, in_gain, left_weight, right_weight, mid_gain, out_weight, out_gate):
    ready, left, right = project_pair(pair_rows, in_gain, left_weight, right_weight)
    left, right = lax.optimization_barrier((left, right))

    def one_channel(pair_of):
        return (jnp.dot(pair_of[0].T, pair_of[1], preferred_element_type=jnp.float32) * RESIDUES ** (-0.5)).astype(jnp.bfloat16)
    mixed = jnp.moveaxis(lax.map(one_channel, (jnp.moveaxis(left, -1, 0), jnp.moveaxis(right, -1, 0))), 0, -1)
    mixed = lax.optimization_barrier(mixed)
    return to_pair(mixed, ready, mid_gain, out_weight, out_gate)
```

```python
import functools

import jax
import jax.numpy as jnp
from jax import lax
from jax.experimental import pallas as pl
from jax.experimental.pallas import tpu as pltpu
from jax.sharding import PartitionSpec as P

MESH = pl.DeviceIdType.MESH


def norm_channels(values, channel_gain):
    centred = values - jnp.mean(values, axis=-1, keepdims=True)
    return (
        centred
        * lax.rsqrt(jnp.mean(centred * centred, axis=-1, keepdims=True) + 1e-05)
        * channel_gain
    )


def flip(index, bits, count):
    out, weight = 0, 1
    while weight < count:
        out = out + weight * lax.rem(lax.div(index, weight) + (bits // weight) % 2, 2)
        weight *= 2
    return out


def dot(a, b):
    return jnp.dot(a, b, preferred_element_type=jnp.float32)


def triangle_kernel(
    rows, cols, planes, lines,
    x_ref, in_gain_ref, left_w_ref, right_w_ref, mid_gain_ref, out_w_ref, gate_w_ref,
    out_ref,
    split, lsend, lrecv, rsend, rrecv, left32, right32, own, psend, precv, gate,
    lsend_sem, lrecv_sem, rsend_sem, rrecv_sem, psend_sem, precv_sem,
):
    first, second = lax.axis_index("first"), lax.axis_index("second")
    z, core = lax.div(first, 2), lax.rem(first, 2)
    pairs = rows * cols
    half = cols // 2

    def device(z_at, core_at, second_at):
        return {"first": 2 * z_at + core_at, "second": second_at}

    barrier = pltpu.get_barrier_semaphore()
    peers = 0
    for t in range(lines):
        for rel in range(2):
            if t or rel:
                to = device(z, lax.rem(core + rel, 2), flip(second, t, lines))
                pl.semaphore_signal(barrier, inc=1, device_id=to, device_id_type=MESH)
                peers += 1
    for dz in range(1, planes):
        to = device(lax.rem(z + dz, planes), core, second)
        pl.semaphore_signal(barrier, inc=1, device_id=to, device_id_type=MESH)
        peers += 1

    ready = norm_channels(x_ref[...].astype(jnp.float32), in_gain_ref[...]).astype(jnp.bfloat16)
    left = dot(ready, left_w_ref[...])
    for k in range(rows):
        for h in range(2):
            at = k * cols + h * half
            split[h, k * half : (k + 1) * half, :] = left[at : at + half, :]
    for h in range(2):
        lsend[h] = split[h].astype(jnp.bfloat16)
    right = dot(ready, right_w_ref[...]).astype(jnp.bfloat16)
    rsend[...] = right

    pl.semaphore_wait(barrier, peers)

    left_copies = {}
    for t in range(lines - 1, -1, -1):
        for rel in range(2):
            if t or rel:
                to_core = lax.rem(core + rel, 2)
                copy = pltpu.make_async_remote_copy(
                    src_ref=lsend.at[to_core],
                    dst_ref=lrecv.at[t, rel],
                    send_sem=lsend_sem.at[t, rel],
                    recv_sem=lrecv_sem.at[t, rel],
                    device_id=device(z, to_core, flip(second, t, lines)),
                    device_id_type=MESH,
                )
                copy.start()
                left_copies[t, rel] = copy
    right_copy = pltpu.make_async_remote_copy(
        src_ref=rsend,
        dst_ref=rrecv,
        send_sem=rsend_sem,
        recv_sem=rrecv_sem,
        device_id=device(z, 1 - core, second),
        device_id_type=MESH,
    )
    right_copy.start()

    gate[...] = jax.nn.sigmoid(dot(ready, gate_w_ref[...]))
    right32[0] = right.astype(jnp.float32)
    right_copy.wait_recv()
    right32[1] = rrecv[...].astype(jnp.float32)

    part_copies = []
    for t in range(lines):
        for rel in range(2):
            if t or rel:
                left_copies[t, rel].wait_recv()
                left32[rel] = lrecv[t, rel].astype(jnp.float32)
            else:
                left32[rel] = lsend[core].astype(jnp.float32)

        sums = tuple(jnp.zeros((cols, x_ref.shape[1]), jnp.float32) for _ in range(half))
        for rel in range(2):

            def body(k, sums):
                r = right32[rel, pl.ds(pl.multiple_of(k * cols, 8), cols), :]
                return tuple(
                    total + left32[rel, pl.ds(k * half + i, 1), :] * r
                    for i, total in enumerate(sums)
                )

            sums = lax.fori_loop(0, rows, body, sums)

        z_to = flip(second, t, lines)
        is_own = z_to == z

        @pl.when(is_own)
        def _():
            for i, total in enumerate(sums):
                own[i * cols : (i + 1) * cols, :] = total

        for i in range(0, half, 2):
            two = jnp.concatenate([sums[i], sums[i + 1]], axis=0)
            psend[t, i * cols : (i + 2) * cols, :] = two.astype(jnp.bfloat16)
        slot = lax.rem(z - z_to + 2 * planes - 1, planes)
        copy = pltpu.make_async_remote_copy(
            src_ref=psend.at[t],
            dst_ref=precv.at[slot],
            send_sem=psend_sem.at[t],
            recv_sem=precv_sem.at[slot],
            device_id=device(z_to, core, second),
            device_id_type=MESH,
        )
        part_copies.append((is_own, copy))

        @pl.when(jnp.logical_not(is_own))
        def _():
            copy.start()

    total = own[...]
    for slot in range(planes - 1):
        pltpu.make_async_remote_copy(
            src_ref=psend.at[0],
            dst_ref=precv.at[slot],
            send_sem=psend_sem.at[0],
            recv_sem=precv_sem.at[slot],
            device_id=device(lax.rem(z + 1, planes), core, second),
            device_id_type=MESH,
        ).wait_recv()
        total = total + precv[slot].astype(jnp.float32)
    count = rows * 2 * planes
    mixed = (total * count ** (-0.5)).astype(jnp.bfloat16)
    scaled = norm_channels(mixed.astype(jnp.float32), mid_gain_ref[...]).astype(jnp.bfloat16)
    out_ref[...] = (dot(scaled, out_w_ref[...]) * gate[...]).astype(jnp.bfloat16)

    for copy in left_copies.values():
        copy.wait_send()
    right_copy.wait_send()
    for is_own, copy in part_copies:

        @pl.when(jnp.logical_not(is_own))
        def _():
            copy.wait_send()


def triangle(planes, lines, pair_rows, in_gain, left_weight, right_weight, mid_gain, out_weight, out_gate):
    rows, cols, width = pair_rows.shape
    mix = left_weight.shape[1]
    pairs, half = rows * cols, cols // 2
    vmem = pl.BlockSpec(memory_space=pltpu.VMEM)
    bf16, f32 = jnp.bfloat16, jnp.float32
    out = pl.pallas_call(
        functools.partial(triangle_kernel, rows, cols, planes, lines),
        out_shape=pltpu.VMEM((pairs, width), bf16),
        in_specs=[vmem] * 7,
        out_specs=vmem,
        scratch_shapes=[
            pltpu.VMEM((2, rows * half, mix), f32),
            pltpu.VMEM((2, rows * half, mix), bf16),
            pltpu.VMEM((lines, 2, rows * half, mix), bf16),
            pltpu.VMEM((pairs, mix), bf16),
            pltpu.VMEM((pairs, mix), bf16),
            pltpu.VMEM((2, rows * half, mix), f32),
            pltpu.VMEM((2, pairs, mix), f32),
            pltpu.VMEM((half * cols, mix), f32),
            pltpu.VMEM((lines, half * cols, mix), bf16),
            pltpu.VMEM((planes - 1, half * cols, mix), bf16),
            pltpu.VMEM((pairs, width), f32),
            pltpu.SemaphoreType.DMA((lines, 2)),
            pltpu.SemaphoreType.DMA((lines, 2)),
            pltpu.SemaphoreType.DMA,
            pltpu.SemaphoreType.DMA,
            pltpu.SemaphoreType.DMA((lines,)),
            pltpu.SemaphoreType.DMA((planes - 1,)),
        ],
        compiler_params=pltpu.CompilerParams(collective_id=0, has_side_effects=True),
    )(
        pair_rows.reshape(pairs, width), in_gain.reshape(1, width), left_weight, right_weight,
        mid_gain.reshape(1, mix), out_weight, out_gate,
    )
    return out.reshape(rows, cols, width)


def shards(pair_rows, in_gain, left_weight, right_weight, mid_gain, out_weight, out_gate):
    ready = norm_channels(pair_rows.astype(jnp.float32), in_gain).astype(jnp.bfloat16)
    ready = lax.optimization_barrier(ready)
    left = jnp.einsum("ijc,cd->ijd", ready, left_weight, preferred_element_type=jnp.float32)
    right = jnp.einsum("ijc,cd->ijd", ready, right_weight, preferred_element_type=jnp.float32)
    left, right = left.astype(jnp.bfloat16), right.astype(jnp.bfloat16)
    count = pair_rows.shape[0] * lax.axis_size("first")
    left_lines, right_lines = (
        lax.all_to_all(left, "first", split_axis=2, concat_axis=0, tiled=True),
        lax.all_to_all(right, "first", split_axis=2, concat_axis=0, tiled=True),
    )
    strip = jnp.einsum(
        "kid,kjd->ijd",
        lax.all_gather(left_lines, "second", axis=1, tiled=True),
        right_lines,
        preferred_element_type=jnp.float32,
    )
    strip = (strip * count ** (-0.5)).astype(jnp.bfloat16)
    mixed = lax.all_to_all(strip, "first", split_axis=0, concat_axis=2, tiled=True)
    scaled = norm_channels(mixed.astype(jnp.float32), mid_gain).astype(jnp.bfloat16)
    scaled = lax.optimization_barrier(scaled)
    gate = jax.nn.sigmoid(
        jnp.einsum("ijc,cd->ijd", ready, out_gate, preferred_element_type=jnp.float32)
    )
    return (
        jnp.einsum("ijd,dc->ijc", scaled, out_weight, preferred_element_type=jnp.float32) * gate
    ).astype(jnp.bfloat16)


def solution(mesh):
    in_specs = (P("first", "second", None), P(), P(), P(), P(), P(), P())
    out_specs = P("first", "second", None)
    planes, lines = mesh.shape["first"] // 2, mesh.shape["second"]
    if mesh.shape["first"] == 2 * lines and lines & (lines - 1) == 0:
        body = functools.partial(triangle, planes, lines)
    else:
        body = shards
    return jax.shard_map(body, mesh=mesh, in_specs=in_specs, out_specs=out_specs, check_vma=False)
```

```python
import functools

import jax
import jax.numpy as jnp
from jax import lax
from jax.experimental import pallas as pl
from jax.experimental.pallas import tpu as pltpu
from jax.sharding import PartitionSpec as P

MESH = pl.DeviceIdType.MESH


def norm_channels(values, channel_gain):
    centred = values - jnp.mean(values, axis=-1, keepdims=True)
    return (
        centred
        * lax.rsqrt(jnp.mean(centred * centred, axis=-1, keepdims=True) + 1e-05)
        * channel_gain
    )


def flip(index, bits, count):
    out, weight = 0, 1
    while weight < count:
        out = out + weight * lax.rem(lax.div(index, weight) + (bits // weight) % 2, 2)
        weight *= 2
    return out


def dot(a, b):
    return jnp.dot(a, b, preferred_element_type=jnp.float32)


CHUNK = 4


def flip_low(index):
    return index + 1 - 2 * lax.rem(index, 2)


def triangle_kernel(
    rows, cols, planes, lines,
    x_hbm, in_gain_hbm, left_w_hbm, right_w_hbm, mid_gain_hbm, out_w_hbm, gate_w_hbm,
    out_ref,
    x_ref, in_gain_ref, left_w_ref, right_w_ref, mid_gain_ref, out_w_ref, gate_w_ref,
    lsend, lrecv, rsend, left32, right32, psend, part32, inbox, gate,
    in_sem, lsend_sem, lrecv_sem, rsend_sem, rrecv_sem, psend_sem, inbox_sem, go_sem,
):
    first, second = lax.axis_index("first"), lax.axis_index("second")
    z, core = lax.div(first, 2), lax.rem(first, 2)
    pairs = rows * cols
    chunks = cols // CHUNK
    per_core = chunks // 2
    size = CHUNK * cols
    half = planes // 2
    upper, side = lax.div(z, half), lax.div(second, half)
    near_z = flip_low(z)
    inner = lax.rem(z, 2) != upper

    def device(z_at, core_at, second_at):
        return {"first": 2 * z_at + core_at, "second": second_at}

    scope = jax.named_scope
    barrier = pltpu.get_barrier_semaphore()

    def greet(to):
        pl.semaphore_signal(barrier, inc=1, device_id=to, device_id_type=MESH)

    with scope("sig"):
        for t in range(lines):
            for rel in range(2):
                if t or rel:
                    greet(device(z, lax.rem(core + rel, 2), flip(second, t, lines)))
        for dz in (1, 2):
            for c in range(2):
                greet(device(flip(z, dz, planes), c, second))

        @pl.when(inner)
        def _():
            for c in range(2):
                greet(device(flip(z, 3, planes), c, second))

    loads = [
        pltpu.make_async_copy(src, dst, in_sem.at[n])
        for n, (src, dst) in enumerate((
            (x_hbm, x_ref), (in_gain_hbm, in_gain_ref), (left_w_hbm, left_w_ref), (right_w_hbm, right_w_ref),
            (gate_w_hbm, gate_w_ref), (mid_gain_hbm, mid_gain_ref), (out_w_hbm, out_w_ref),
        ))
    ]
    for load in loads:
        load.start()
    with scope("load"):
        for load in loads[:3]:
            load.wait()

    with scope("left"):
        ready = norm_channels(x_ref[...].astype(jnp.float32), in_gain_ref[...]).astype(jnp.bfloat16)
        left = dot(ready, left_w_ref[...]).astype(jnp.bfloat16)
        lsend[...] = left
        lrecv[0, core] = left

    with scope("bar"):
        pl.semaphore_wait(barrier, 2 * lines - 1 + 4 + 2 * inner.astype(jnp.int32))

    target = lax.rem(side + upper, 2)

    def left_copy(t):
        return pltpu.make_async_remote_copy(
            src_ref=lsend,
            dst_ref=lrecv.at[t, core],
            send_sem=lsend_sem.at[t],
            recv_sem=lrecv_sem.at[t, core],
            device_id=device(z, target, flip(second, t, lines)),
            device_id_type=MESH,
        )

    for t in (2, 1, 3):
        left_copy(t).start()

    @pl.when(target != core)
    def _():
        left_copy(0).start()

    with scope("right"):
        loads[3].wait()
        right = dot(ready, right_w_ref[...]).astype(jnp.bfloat16)
        rsend[core] = right
    right_copy = pltpu.make_async_remote_copy(
        src_ref=rsend.at[core],
        dst_ref=rsend.at[core],
        send_sem=rsend_sem,
        recv_sem=rrecv_sem,
        device_id=device(z, 1 - core, second),
        device_id_type=MESH,
    )
    right_copy.start()
    with scope("gate"):
        loads[4].wait()
        gate[...] = jax.nn.sigmoid(dot(ready, gate_w_ref[...]))
        loads[5].wait()
        loads[6].wait()
    with scope("rwait"):
        right_copy.wait_recv()
    with scope("r32"):
        for q in range(2):
            right32[q * pairs : (q + 1) * pairs, :] = rsend[q].astype(jnp.float32)

    target_side = jnp.where(core == 1, 1 - upper, upper)
    t_high = lax.rem(side + target_side, 2)

    def block_plane(u):
        return half * target_side + lax.rem(lax.rem(second, 2) + u, 2)

    def send(u, c, slot, to):
        return pltpu.make_async_remote_copy(
            src_ref=psend.at[u, c],
            dst_ref=inbox.at[slot],
            send_sem=psend_sem.at[u, c],
            recv_sem=inbox_sem.at[slot],
            device_id=to,
            device_id_type=MESH,
        )

    near_at, cross_at, own_at = 2 * chunks, 2 * chunks + per_core, 2 * chunks + 2 * per_core
    crossing = core == 1
    outer = jnp.logical_not(inner)
    t_near = 2 * lax.rem(side + upper, 2) + lax.rem(lax.rem(second, 2) + lax.rem(near_z, 2), 2)
    held_back = jnp.logical_and(outer, t_near != 0)

    for u in range(2):
        t_at = half * t_high + u
        plane = block_plane(u)
        is_own = plane == z
        for q in range(2):
            mine = jnp.logical_and(t_at == 0, core == q)

            with scope(f"wl{u}{q}"):

                @pl.when(jnp.logical_not(mine))
                def _():
                    pltpu.make_async_remote_copy(
                        src_ref=lsend,
                        dst_ref=lrecv.at[t_at, q],
                        send_sem=lsend_sem.at[0],
                        recv_sem=lrecv_sem.at[t_at, q],
                        device_id=device(z, 1 - core, second),
                        device_id_type=MESH,
                    ).wait_recv()

            left32[q * pairs : (q + 1) * pairs, :] = lrecv[t_at, q].astype(jnp.float32)

        with scope(f"block{u}"):
            for c in range(chunks):

                def body(k, sums):
                    r = right32[pl.ds(pl.multiple_of(k * cols, 8), cols), :]
                    return tuple(
                        total + left32[pl.ds(k * cols + c * CHUNK + i, 1), :] * r
                        for i, total in enumerate(sums)
                    )

                sums = lax.fori_loop(
                    0, 2 * rows, body,
                    tuple(jnp.zeros((cols, x_ref.shape[1]), jnp.float32) for _ in range(CHUNK)),
                    unroll=8,
                )
                total = jnp.concatenate(sums, axis=0)
                part32[u, c] = total
                psend[u, c] = total.astype(jnp.bfloat16)
                to_core = c // per_core

                @pl.when(jnp.logical_and(crossing, outer))
                def _():
                    send(u, c, u * chunks + c, device(near_z, 1, second)).start()

                if to_core == 1:

                    @pl.when(jnp.logical_and(jnp.logical_not(crossing), is_own))
                    def _():
                        send(u, c, own_at + c % per_core, device(z, 1, second)).start()

                @pl.when(
                    jnp.logical_not(jnp.logical_or(crossing, jnp.logical_or(is_own, held_back)))
                )
                def _():
                    send(u, c, near_at + c % per_core, device(near_z, to_core, second)).start()

    def each(what):
        for u in range(2):
            for c in range(chunks):
                what(u, c, send(u, c, near_at + c % per_core, device(near_z, c // per_core, second)))

    with scope("relay"):

        @pl.when(jnp.logical_and(crossing, inner))
        def _():
            for u in range(2):
                for c in range(chunks):
                    send(u, c, u * chunks + c, device(near_z, 1, second)).wait_recv()
                    total = part32[u, c] + inbox[u * chunks + c].astype(jnp.float32)
                    psend[u, c] = total.astype(jnp.bfloat16)
                    send(
                        u, c, cross_at + c % per_core, device(block_plane(u), c // per_core, second)
                    ).start()

    with scope("held"):

        @pl.when(held_back)
        def _():
            @pl.when(crossing)
            def _():
                each(lambda u, c, copy: copy.wait_send())
                pl.semaphore_signal(go_sem, inc=1, device_id=device(z, 0, second), device_id_type=MESH)

            @pl.when(jnp.logical_not(crossing))
            def _():
                pl.semaphore_wait(go_sem, 1)
                for u in range(2):

                    @pl.when(block_plane(u) != z)
                    def _():
                        for c in range(chunks):
                            send(
                                u, c, near_at + c % per_core, device(near_z, c // per_core, second)
                            ).start()

    own_u = lax.rem(lax.rem(second, 2) + lax.rem(z, 2), 2)
    count = rows * 2 * planes
    for c in range(per_core):
        with scope(f"own{c}"):

            @pl.when(crossing)
            def _():
                send(0, c, own_at + c, device(z, 0, second)).wait_recv()
                part32[0, c] = inbox[own_at + c].astype(jnp.float32)

            at_own = jnp.where(crossing, 0, own_u)
        with scope(f"near{c}"):
            send(0, c, near_at + c, device(near_z, 0, second)).wait_recv()
        with scope(f"cross{c}"):
            send(0, c, cross_at + c, device(near_z, 0, second)).wait_recv()
        with scope(f"final{c}"):
            total = (
                part32[at_own, c]
                + inbox[near_at + c].astype(jnp.float32)
                + inbox[cross_at + c].astype(jnp.float32)
            )
            mixed = (total * count ** (-0.5)).astype(jnp.bfloat16)
            scaled = norm_channels(mixed.astype(jnp.float32), mid_gain_ref[...]).astype(jnp.bfloat16)
            at = slice(c * size, (c + 1) * size)
            out_ref[at, :] = (dot(scaled, out_w_ref[...]) * gate[at, :]).astype(jnp.bfloat16)

    with scope("drain"):
        for t in (1, 2, 3):
            left_copy(t).wait_send()

        @pl.when(target != core)
        def _():
            left_copy(0).wait_send()

        right_copy.wait_send()

        @pl.when(crossing)
        def _():
            @pl.when(jnp.logical_not(held_back))
            def _():
                each(lambda u, c, copy: copy.wait_send())

        @pl.when(jnp.logical_not(crossing))
        def _():
            for u in range(2):

                @pl.when(block_plane(u) != z)
                def _():
                    for c in range(per_core):
                        send(u, c, near_at + c, device(near_z, 0, second)).wait_send()

                for c in range(per_core, chunks):
                    send(u, c, near_at + c - per_core, device(near_z, 1, second)).wait_send()


def triangle(planes, lines, pair_rows, in_gain, left_weight, right_weight, mid_gain, out_weight, out_gate):
    rows, cols, width = pair_rows.shape
    mix = left_weight.shape[1]
    pairs, chunks, size = rows * cols, cols // CHUNK, CHUNK * cols
    slots = 2 * chunks + 3 * (chunks // 2)
    anywhere = pl.BlockSpec(memory_space=pl.ANY)
    bf16, f32 = jnp.bfloat16, jnp.float32
    out = pl.pallas_call(
        functools.partial(triangle_kernel, rows, cols, planes, lines),
        out_shape=pltpu.VMEM((pairs, width), bf16),
        in_specs=[anywhere] * 7,
        out_specs=pl.BlockSpec(memory_space=pltpu.VMEM),
        scratch_shapes=[
            pltpu.VMEM((pairs, width), bf16),
            pltpu.VMEM((1, width), f32),
            pltpu.VMEM((width, mix), bf16),
            pltpu.VMEM((width, mix), bf16),
            pltpu.VMEM((1, mix), f32),
            pltpu.VMEM((mix, width), bf16),
            pltpu.VMEM((width, width), bf16),
            pltpu.VMEM((pairs, mix), bf16),
            pltpu.VMEM((lines, 2, pairs, mix), bf16),
            pltpu.VMEM((2, pairs, mix), bf16),
            pltpu.VMEM((2 * pairs, mix), f32),
            pltpu.VMEM((2 * pairs, mix), f32),
            pltpu.VMEM((2, chunks, size, mix), bf16),
            pltpu.VMEM((2, chunks, size, mix), f32),
            pltpu.VMEM((slots, size, mix), bf16),
            pltpu.VMEM((pairs, width), f32),
            pltpu.SemaphoreType.DMA((7,)),
            pltpu.SemaphoreType.DMA((lines,)),
            pltpu.SemaphoreType.DMA((lines, 2)),
            pltpu.SemaphoreType.DMA,
            pltpu.SemaphoreType.DMA,
            pltpu.SemaphoreType.DMA((2, chunks)),
            pltpu.SemaphoreType.DMA((slots,)),
            pltpu.SemaphoreType.REGULAR,
        ],
        compiler_params=pltpu.CompilerParams(collective_id=0, has_side_effects=True),
    )(
        pair_rows.reshape(pairs, width), in_gain.reshape(1, width), left_weight, right_weight,
        mid_gain.reshape(1, mix), out_weight, out_gate,
    )
    return out.reshape(rows, cols, width)


def shards(pair_rows, in_gain, left_weight, right_weight, mid_gain, out_weight, out_gate):
    ready = norm_channels(pair_rows.astype(jnp.float32), in_gain).astype(jnp.bfloat16)
    ready = lax.optimization_barrier(ready)
    left = jnp.einsum("ijc,cd->ijd", ready, left_weight, preferred_element_type=jnp.float32)
    right = jnp.einsum("ijc,cd->ijd", ready, right_weight, preferred_element_type=jnp.float32)
    left, right = left.astype(jnp.bfloat16), right.astype(jnp.bfloat16)
    count = pair_rows.shape[0] * lax.axis_size("first")
    left_lines, right_lines = (
        lax.all_to_all(left, "first", split_axis=2, concat_axis=0, tiled=True),
        lax.all_to_all(right, "first", split_axis=2, concat_axis=0, tiled=True),
    )
    strip = jnp.einsum(
        "kid,kjd->ijd",
        lax.all_gather(left_lines, "second", axis=1, tiled=True),
        right_lines,
        preferred_element_type=jnp.float32,
    )
    strip = (strip * count ** (-0.5)).astype(jnp.bfloat16)
    mixed = lax.all_to_all(strip, "first", split_axis=0, concat_axis=2, tiled=True)
    scaled = norm_channels(mixed.astype(jnp.float32), mid_gain).astype(jnp.bfloat16)
    scaled = lax.optimization_barrier(scaled)
    gate = jax.nn.sigmoid(
        jnp.einsum("ijc,cd->ijd", ready, out_gate, preferred_element_type=jnp.float32)
    )
    return (
        jnp.einsum("ijd,dc->ijc", scaled, out_weight, preferred_element_type=jnp.float32) * gate
    ).astype(jnp.bfloat16)


def solution(mesh):
    in_specs = (P("first", "second", None), P(), P(), P(), P(), P(), P())
    out_specs = P("first", "second", None)
    planes, lines = mesh.shape["first"] // 2, mesh.shape["second"]
    if planes == lines == 4:
        body = functools.partial(triangle, planes, lines)
    else:
        body = shards
    return jax.shard_map(body, mesh=mesh, in_specs=in_specs, out_specs=out_specs, check_vma=False)
```

```python
import functools

import jax
import jax.numpy as jnp
from jax import lax
from jax.experimental import pallas as pl
from jax.experimental.pallas import tpu as pltpu
from jax.sharding import PartitionSpec as P

MESH = pl.DeviceIdType.MESH


def norm_channels(values, channel_gain):
    centred = values - jnp.mean(values, axis=-1, keepdims=True)
    return (
        centred
        * lax.rsqrt(jnp.mean(centred * centred, axis=-1, keepdims=True) + 1e-05)
        * channel_gain
    )


def dot(a, b):
    return jnp.dot(a, b, preferred_element_type=jnp.float32)


PIECE = 8
CHUNK = 4


def other(index):
    return index + 1 - 2 * lax.rem(index, 2)


def triangle_kernel(
    rows, cols, planes, lines,
    x_hbm, in_gain_hbm, left_w_hbm, right_w_hbm, mid_gain_hbm, out_w_hbm, gate_w_hbm,
    out_ref,
    x_ref, in_gain_ref, left_w_ref, right_w_ref, mid_gain_ref, out_w_ref, gate_w_ref,
    lsend, lrecv, rboth, left32, right32, psend, part32, inbox, gate,
    in_sem, lsend_sem, lrecv_sem, rsend_sem, rrecv_sem, psend_sem, inbox_sem, go_sem,
):
    first, second = lax.axis_index("first"), lax.axis_index("second")
    z, core = lax.div(first, 2), lax.rem(first, 2)
    pieces, chunks = cols // PIECE, cols // CHUNK
    per_piece, per_core = PIECE // CHUNK, chunks // 2
    lump, size = rows * PIECE, CHUNK * cols
    half = planes // 2
    upper, side, parity = lax.div(z, half), lax.div(second, half), lax.rem(second, 2)
    near_z = other(z)
    inner = lax.rem(z, 2) != upper
    outer = jnp.logical_not(inner)
    crossing = core == 1
    level = core == 0
    target_side = jnp.where(crossing, 1 - upper, upper)
    planes_of = [half * target_side + lax.rem(parity + u, 2) for u in range(2)]
    from_own = target_side == side
    is_own = [jnp.logical_and(level, planes_of[u] == z) for u in range(2)]
    is_near = [jnp.logical_and(level, planes_of[u] != z) for u in range(2)]
    x_second, y_second = other(second), lax.rem(second + half, lines)
    xy_second = other(y_second)
    cross_z = 2 * lax.rem(upper + 1, 2) + lax.rem(upper + 1 + 1, 2)

    def device(z_at, core_at, second_at):
        return {"first": 2 * z_at + core_at, "second": second_at}

    scope = jax.named_scope
    barrier = pltpu.get_barrier_semaphore()

    def greet(z_at, core_at, second_at):
        pl.semaphore_signal(
            barrier, inc=1, device_id=device(z_at, core_at, second_at), device_id_type=MESH
        )

    with scope("sig"):
        greet(z, 1 - core, second)
        for c in range(2):

            @pl.when(from_own)
            def _():
                greet(z, c, x_second)

            @pl.when(jnp.logical_not(from_own))
            def _():
                greet(z, c, y_second)
                greet(z, c, xy_second)

        @pl.when(jnp.logical_and(crossing, inner))
        def _():
            greet(near_z, 1, second)

        greet(near_z, 0, second)
        greet(cross_z, 1, second)

    loads = [
        pltpu.make_async_copy(src, dst, in_sem.at[n])
        for n, (src, dst) in enumerate((
            (x_hbm, x_ref), (in_gain_hbm, in_gain_ref), (left_w_hbm, left_w_ref), (right_w_hbm, right_w_ref),
            (gate_w_hbm, gate_w_ref), (mid_gain_hbm, mid_gain_ref), (out_w_hbm, out_w_ref),
        ))
    ]
    for load in loads:
        load.start()
    with scope("loadx"):
        loads[0].wait()
    with scope("loadw"):
        loads[1].wait()
        loads[2].wait()

    target = lax.rem(side + upper, 2)

    def left_copy(t, c):
        return pltpu.make_async_remote_copy(
            src_ref=lsend.at[c],
            dst_ref=lrecv.at[t % 2, core, c],
            send_sem=lsend_sem.at[t, c],
            recv_sem=lrecv_sem.at[t % 2, core, c],
            device_id=device(z, target, (second, x_second, y_second, xy_second)[t]),
            device_id_type=MESH,
        )

    with scope("left"):
        x = x_ref[...].astype(jnp.float32)
        ready = []
        for c in range(pieces):
            lump_of = jnp.concatenate(
                [x[k * cols + c * PIECE : k * cols + (c + 1) * PIECE, :] for k in range(rows)], axis=0
            )
            ready.append(norm_channels(lump_of, in_gain_ref[...]).astype(jnp.bfloat16))
            left = dot(ready[c], left_w_ref[...]).astype(jnp.bfloat16)
            lsend[c] = left

    with scope("bar"):
        pl.semaphore_wait(
            barrier,
            jnp.where(level, 6, jnp.where(outer, 5, 8)).astype(jnp.int32),
        )

    @pl.when(target != core)
    def _():
        for c in range(pieces):
            left_copy(0, c).start()

    for c in range(pieces):
        for t in (2, 1, 3):
            left_copy(t, c).start()

    with scope("right"):
        loads[3].wait()
        ready = jnp.concatenate(ready, axis=0)
        right = dot(ready, right_w_ref[...]).astype(jnp.bfloat16)
        rboth[core] = right

    right_copy = pltpu.make_async_remote_copy(
        src_ref=rboth.at[core],
        dst_ref=rboth.at[core],
        send_sem=rsend_sem,
        recv_sem=rrecv_sem,
        device_id=device(z, 1 - core, second),
        device_id_type=MESH,
    )
    right_copy.start()
    with scope("gate"):
        loads[4].wait()
        gates = jax.nn.sigmoid(dot(ready, gate_w_ref[...]))
        for c in range(pieces):
            for k in range(rows):
                at = c * lump + k * PIECE
                gate[k * cols + c * PIECE : k * cols + (c + 1) * PIECE, :] = gates[at : at + PIECE, :]
        loads[5].wait()
        loads[6].wait()

    with scope("rwait"):
        right_copy.wait_recv()
    with scope("r32"):
        for q in range(2):
            right32[q] = rboth[q].astype(jnp.float32)

    def send(j, n, slot, to):
        return pltpu.make_async_remote_copy(
            src_ref=psend.at[j, n],
            dst_ref=inbox.at[slot],
            send_sem=psend_sem.at[j, n],
            recv_sem=inbox_sem.at[slot],
            device_id=to,
            device_id_type=MESH,
        )

    near_at, cross_at, own_at = 2 * chunks, 2 * chunks + per_core, 2 * chunks + 2 * per_core
    near_early = jnp.logical_and(upper == side, parity != lax.rem(z, 2))
    held_back = jnp.logical_and(outer, jnp.logical_not(near_early))

    def relay_copy(j, n):
        return send(j, n, j * chunks + n, device(near_z, 1, second))

    def near_copy(j, n):
        return send(j, n, near_at + n % per_core, device(near_z, n // per_core, second))

    def cross_copy(j, n):
        return send(j, n, cross_at + n % per_core, device(planes_of[j], n // per_core, second))

    def own_copy(j, n):
        return send(j, n, own_at + n % per_core, device(z, 1, second))

    def block(j, c):
        with scope(f"wl{j}{c}"):
            for q in range(2):
                mine = jnp.logical_and(from_own, core == q) if j == 0 else None

                def arrived():
                    pltpu.make_async_remote_copy(
                        src_ref=lsend.at[c],
                        dst_ref=lrecv.at[j, q, c],
                        send_sem=lsend_sem.at[0, c],
                        recv_sem=lrecv_sem.at[j, q, c],
                        device_id=device(z, 1 - core, second),
                        device_id_type=MESH,
                    ).wait_recv()
                    left32[c, q] = lrecv[j, q, c].astype(jnp.float32)

                if j:
                    arrived()
                else:
                    pl.when(jnp.logical_not(mine))(arrived)

                    @pl.when(mine)
                    def _():
                        left32[c, q] = lsend[c].astype(jnp.float32)

        with scope(f"block{j}{c}"):
            for part in range(per_piece):
                n = c * per_piece + part
                sums = tuple(jnp.zeros((cols, x_ref.shape[1]), jnp.float32) for _ in range(CHUNK))
                for q in range(2):

                    def body(k, sums):
                        at = pl.multiple_of(k * PIECE, PIECE)
                        r = jnp.concatenate(
                            [right32[q, pl.ds(p * lump + at, PIECE), :] for p in range(pieces)], axis=0
                        )
                        return tuple(
                            total + left32[c, q, pl.ds(at + part * CHUNK + i, 1), :] * r
                            for i, total in enumerate(sums)
                        )

                    sums = lax.fori_loop(0, rows, body, sums, unroll=True)
                total = jnp.concatenate(sums, axis=0)

                @pl.when(jnp.logical_and(crossing, inner))
                def _():
                    part32[j, n] = total

                psend[j, n] = total.astype(jnp.bfloat16)

                @pl.when(jnp.logical_and(crossing, outer))
                def _():
                    relay_copy(j, n).start()

                @pl.when(is_own[j])
                def _():
                    if n < per_core:
                        inbox[own_at + n] = psend[j, n]
                    else:
                        own_copy(j, n).start()

                @pl.when(jnp.logical_and(is_near[j], jnp.logical_not(held_back)))
                def _():
                    near_copy(j, n).start()

    @pl.when(from_own)
    def _():
        for j in range(2):
            for c in range(pieces):
                block(j, c)

    @pl.when(jnp.logical_not(from_own))
    def _():
        for c in range(pieces):
            for j in range(2):
                block(j, c)

    everything = [
        (j, c * per_piece + part) for c in range(pieces) for j in range(2) for part in range(per_piece)
    ]
    with scope("relay"):

        @pl.when(jnp.logical_and(crossing, inner))
        def _():
            for j, n in everything:
                relay_copy(j, n).wait_recv()
                total = part32[j, n] + inbox[j * chunks + n].astype(jnp.float32)
                psend[j, n] = total.astype(jnp.bfloat16)
                cross_copy(j, n).start()

    with scope("held"):

        @pl.when(held_back)
        def _():
            @pl.when(crossing)
            def _():
                for j, n in everything:
                    relay_copy(j, n).wait_send()
                pl.semaphore_signal(go_sem, inc=1, device_id=device(z, 0, second), device_id_type=MESH)

            @pl.when(level)
            def _():
                pl.semaphore_wait(go_sem, 1)
                for j in range(2):

                    @pl.when(is_near[j])
                    def _():
                        for n in range(chunks):
                            near_copy(j, n).start()

    count = rows * 2 * planes
    for c in range(per_core):
        with scope(f"own{c}"):

            @pl.when(crossing)
            def _():
                own_copy(0, c).wait_recv()

        with scope(f"near{c}"):
            near_copy(0, c).wait_recv()
    for group in (range(per_core - 1), (per_core - 1,)):
        with scope(f"cross{group[0]}"):
            for c in group:
                cross_copy(0, c).wait_recv()
        with scope(f"final{group[0]}"):
            total = jnp.concatenate(
                [
                    inbox[own_at + c].astype(jnp.float32)
                    + inbox[near_at + c].astype(jnp.float32)
                    + inbox[cross_at + c].astype(jnp.float32)
                    for c in group
                ],
                axis=0,
            )
            mixed = (total * count ** (-0.5)).astype(jnp.bfloat16)
            scaled = norm_channels(mixed.astype(jnp.float32), mid_gain_ref[...]).astype(jnp.bfloat16)
            at = slice(group[0] * size, (group[-1] + 1) * size)
            out_ref[at, :] = (dot(scaled, out_w_ref[...]) * gate[at, :]).astype(jnp.bfloat16)

    with scope("drain"):
        for t in (1, 2, 3):
            for c in range(pieces):
                left_copy(t, c).wait_send()

        @pl.when(target != core)
        def _():
            for c in range(pieces):
                left_copy(0, c).wait_send()

        right_copy.wait_send()

        @pl.when(jnp.logical_and(crossing, jnp.logical_not(held_back)))
        def _():
            for j, n in everything:
                relay_copy(j, n).wait_send()

        @pl.when(level)
        def _():
            for j, n in everything:
                if n < per_core:

                    @pl.when(is_near[j])
                    def _():
                        near_copy(j, n).wait_send()

                else:
                    near_copy(j, n).wait_send()


def triangle(planes, lines, pair_rows, in_gain, left_weight, right_weight, mid_gain, out_weight, out_gate):
    rows, cols, width = pair_rows.shape
    mix = left_weight.shape[1]
    pairs, pieces, chunks, size = rows * cols, cols // PIECE, cols // CHUNK, CHUNK * cols
    lump = rows * PIECE
    slots = 2 * chunks + 3 * (chunks // 2)
    anywhere = pl.BlockSpec(memory_space=pl.ANY)
    bf16, f32 = jnp.bfloat16, jnp.float32
    out = pl.pallas_call(
        functools.partial(triangle_kernel, rows, cols, planes, lines),
        out_shape=pltpu.VMEM((pairs, width), bf16),
        in_specs=[anywhere] * 7,
        out_specs=pl.BlockSpec(memory_space=pltpu.VMEM),
        scratch_shapes=[
            pltpu.VMEM((pairs, width), bf16),
            pltpu.VMEM((1, width), f32),
            pltpu.VMEM((width, mix), bf16),
            pltpu.VMEM((width, mix), bf16),
            pltpu.VMEM((1, mix), f32),
            pltpu.VMEM((mix, width), bf16),
            pltpu.VMEM((width, width), bf16),
            pltpu.VMEM((pieces, lump, mix), bf16),
            pltpu.VMEM((2, 2, pieces, lump, mix), bf16),
            pltpu.VMEM((2, pairs, mix), bf16),
            pltpu.VMEM((pieces, 2, lump, mix), f32),
            pltpu.VMEM((2, pairs, mix), f32),
            pltpu.VMEM((2, chunks, size, mix), bf16),
            pltpu.VMEM((2, chunks, size, mix), f32),
            pltpu.VMEM((slots, size, mix), bf16),
            pltpu.VMEM((pairs, width), f32),
            pltpu.SemaphoreType.DMA((7,)),
            pltpu.SemaphoreType.DMA((lines, pieces)),
            pltpu.SemaphoreType.DMA((2, 2, pieces)),
            pltpu.SemaphoreType.DMA,
            pltpu.SemaphoreType.DMA,
            pltpu.SemaphoreType.DMA((2, chunks)),
            pltpu.SemaphoreType.DMA((slots,)),
            pltpu.SemaphoreType.REGULAR,
        ],
        compiler_params=pltpu.CompilerParams(collective_id=0, has_side_effects=True),
    )(
        pair_rows.reshape(pairs, width), in_gain.reshape(1, width), left_weight, right_weight,
        mid_gain.reshape(1, mix), out_weight, out_gate,
    )
    return out.reshape(rows, cols, width)


def shards(pair_rows, in_gain, left_weight, right_weight, mid_gain, out_weight, out_gate):
    ready = norm_channels(pair_rows.astype(jnp.float32), in_gain).astype(jnp.bfloat16)
    ready = lax.optimization_barrier(ready)
    left = jnp.einsum("ijc,cd->ijd", ready, left_weight, preferred_element_type=jnp.float32)
    right = jnp.einsum("ijc,cd->ijd", ready, right_weight, preferred_element_type=jnp.float32)
    left, right = left.astype(jnp.bfloat16), right.astype(jnp.bfloat16)
    count = pair_rows.shape[0] * lax.axis_size("first")
    left_lines, right_lines = (
        lax.all_to_all(left, "first", split_axis=2, concat_axis=0, tiled=True),
        lax.all_to_all(right, "first", split_axis=2, concat_axis=0, tiled=True),
    )
    strip = jnp.einsum(
        "kid,kjd->ijd",
        lax.all_gather(left_lines, "second", axis=1, tiled=True),
        right_lines,
        preferred_element_type=jnp.float32,
    )
    strip = (strip * count ** (-0.5)).astype(jnp.bfloat16)
    mixed = lax.all_to_all(strip, "first", split_axis=0, concat_axis=2, tiled=True)
    scaled = norm_channels(mixed.astype(jnp.float32), mid_gain).astype(jnp.bfloat16)
    scaled = lax.optimization_barrier(scaled)
    gate = jax.nn.sigmoid(
        jnp.einsum("ijc,cd->ijd", ready, out_gate, preferred_element_type=jnp.float32)
    )
    return (
        jnp.einsum("ijd,dc->ijc", scaled, out_weight, preferred_element_type=jnp.float32) * gate
    ).astype(jnp.bfloat16)


def solution(mesh):
    in_specs = (P("first", "second", None), P(), P(), P(), P(), P(), P())
    out_specs = P("first", "second", None)
    planes, lines = mesh.shape["first"] // 2, mesh.shape["second"]
    if planes == lines == 4:
        body = functools.partial(triangle, planes, lines)
    else:
        body = shards
    return jax.shard_map(body, mesh=mesh, in_specs=in_specs, out_specs=out_specs, check_vma=False)
```

```python
import functools

import jax
import jax.numpy as jnp
from jax import lax
from jax.experimental import pallas as pl
from jax.experimental.pallas import tpu as pltpu
from jax.sharding import PartitionSpec as P

MESH = pl.DeviceIdType.MESH


def norm_channels(values, channel_gain):
    centred = values - jnp.mean(values, axis=-1, keepdims=True)
    return (
        centred
        * lax.rsqrt(jnp.mean(centred * centred, axis=-1, keepdims=True) + 1e-05)
        * channel_gain
    )


def dot(a, b):
    return jnp.dot(a, b, preferred_element_type=jnp.float32)


PIECE = 8
CHUNK = 4


def other(index):
    return index + 1 - 2 * lax.rem(index, 2)


def centre(values, channel_gain):
    centred = values - jnp.mean(values, axis=-1, keepdims=True)
    scale = lax.rsqrt(jnp.mean(centred * centred, axis=-1, keepdims=True) + 1e-05)
    return (centred * channel_gain).astype(jnp.bfloat16), scale


def triangle_kernel(rows, cols, planes, lines, *refs):
    pieces, chunks = cols // PIECE, cols // CHUNK
    pl.run_scoped(
        functools.partial(triangle_steps, rows, cols, planes, lines, *refs),
        pltpu.SemaphoreType.DMA((6 + pieces,)),
        pltpu.SemaphoreType.DMA((lines, pieces)),
        pltpu.SemaphoreType.DMA((2, 2, pieces)),
        pltpu.SemaphoreType.DMA,
        pltpu.SemaphoreType.DMA,
        pltpu.SemaphoreType.DMA((2, chunks)),
        pltpu.SemaphoreType.DMA((2 * chunks + 3 * (chunks // 2),)),
        pltpu.SemaphoreType.REGULAR,
        pltpu.SemaphoreType.REGULAR,
        pltpu.SemaphoreType.REGULAR,
        pltpu.SemaphoreType.REGULAR,
    )


def triangle_steps(
    rows, cols, planes, lines,
    x_hbm, in_gain_hbm, left_w_hbm, right_w_hbm, mid_gain_hbm, out_w_hbm, gate_w_hbm,
    out_ref,
    x_ref, in_gain_ref, left_w_ref, right_w_ref, mid_gain_ref, out_w_ref, gate_w_ref,
    lsend, lrecv, rboth, left32, right32, psend, part32, inbox, gate,
    in_sem, lsend_sem, lrecv_sem, rsend_sem, rrecv_sem, psend_sem, inbox_sem, go_sem, across_sem, cross_sem, near_sem,
):
    first, second = lax.axis_index("first"), lax.axis_index("second")
    z, core = lax.div(first, 2), lax.rem(first, 2)
    pieces, chunks = cols // PIECE, cols // CHUNK
    per_piece, per_core = PIECE // CHUNK, chunks // 2
    lump, size = rows * PIECE, CHUNK * cols
    half = planes // 2
    upper, side, parity = lax.div(z, half), lax.div(second, half), lax.rem(second, 2)
    near_z = other(z)
    inner = lax.rem(z, 2) != upper
    outer = jnp.logical_not(inner)
    crossing = core == 1
    level = core == 0
    target_side = jnp.where(crossing, 1 - upper, upper)
    planes_of = [half * target_side + lax.rem(parity + u, 2) for u in range(2)]
    from_own = target_side == side
    is_own = [jnp.logical_and(level, planes_of[u] == z) for u in range(2)]
    is_near = [jnp.logical_and(level, planes_of[u] != z) for u in range(2)]
    x_second, y_second = other(second), lax.rem(second + half, lines)
    xy_second = other(y_second)
    cross_z = 2 * lax.rem(upper + 1, 2) + lax.rem(upper + 1 + 1, 2)

    def device(z_at, core_at, second_at):
        return {"first": 2 * z_at + core_at, "second": second_at}

    scope = jax.named_scope
    barrier = pltpu.get_barrier_semaphore()

    def greet(z_at, core_at, second_at):
        pl.semaphore_signal(
            barrier, inc=1, device_id=device(z_at, core_at, second_at), device_id_type=MESH
        )

    target = lax.rem(side + upper, 2)
    early = jnp.logical_and(crossing, jnp.logical_and(inner, upper == 0))
    even = lax.rem(z, 2) == 0

    with scope("sig"):
        greet(z, 1 - core, second)
        for c in range(2):

            @pl.when(from_own)
            def _():
                greet(z, c, x_second)

            @pl.when(jnp.logical_not(from_own))
            def _():
                greet(z, c, y_second)

        @pl.when(side == 0)
        def _():
            greet(z, target, xy_second)

            @pl.when(jnp.logical_not(from_own))
            def _():
                for c in range(2):
                    greet(z, c, xy_second)

        @pl.when(even)
        def _():
            greet(near_z, 0, second)

            @pl.when(level)
            def _():
                for c in range(2):
                    greet(near_z, c, second)

            @pl.when(crossing)
            def _():
                greet(near_z, 1, second)

        @pl.when(upper == 0)
        def _():
            greet(cross_z, 1, second)

        @pl.when(early)
        def _():
            for dz in range(half):
                for c in range(2):
                    greet(half + dz, c, second)

    loads = [
        pltpu.make_async_copy(src, dst, in_sem.at[n])
        for n, (src, dst) in enumerate((
            (in_gain_hbm, in_gain_ref), (left_w_hbm, left_w_ref),
            *((x_hbm.at[:, pl.ds(c * PIECE, PIECE), :], x_ref.at[c]) for c in range(pieces)),
            (right_w_hbm, right_w_ref),
            (gate_w_hbm, gate_w_ref), (mid_gain_hbm, mid_gain_ref), (out_w_hbm, out_w_ref),
        ))
    ]
    for load in loads:
        load.start()
    def meet():
        signals = (
            3
            + jnp.where(even, 0, 1 + jnp.where(level, 2, 1))
            + jnp.where(jnp.logical_and(crossing, z == half), 2 * half, 0)
            + jnp.where(side == 0, 0, 1 + jnp.where(from_own, 0, 2))
            + upper
        )
        pl.semaphore_wait(barrier, signals.astype(jnp.int32))

        def answer(semaphore, z_at, core_at, second_at):
            pl.semaphore_signal(
                semaphore, inc=1, device_id=device(z_at, core_at, second_at), device_id_type=MESH
            )

        @pl.when(jnp.logical_and(side == 1, jnp.logical_not(from_own)))
        def _():
            for c in range(2):
                answer(across_sem, z, c, xy_second)

        @pl.when(jnp.logical_not(even))
        def _():
            answer(near_sem, near_z, 0, second)

        @pl.when(early)
        def _():
            answer(near_sem, near_z, 1, second)

        @pl.when(upper == 1)
        def _():
            answer(cross_sem, cross_z, 1, second)

    with scope("bar"):
        pl.when(side == 1)(meet)

    def left_copy(t, c):
        return pltpu.make_async_remote_copy(
            src_ref=lsend.at[c],
            dst_ref=lrecv.at[t % 2, core, c],
            send_sem=lsend_sem.at[t, c],
            recv_sem=lrecv_sem.at[t % 2, core, c],
            device_id=device(z, target, (second, x_second, y_second, xy_second)[t]),
            device_id_type=MESH,
        )

    with scope("load"):
        loads[0].wait()
        loads[1].wait()

    ready, scales = [], []
    for c in range(pieces):
        with scope(f"left{c}"):
            loads[2 + c].wait()
            x = x_ref[c].astype(jnp.float32).reshape(lump, x_ref.shape[-1])
            for list_of, value in zip((ready, scales), centre(x, in_gain_ref[...])):
                list_of.append(value)
            lsend[c] = (dot(ready[c], left_w_ref[...]) * scales[c]).astype(jnp.bfloat16)
        if c == 0:
            with scope("bar0"):
                pl.when(side == 0)(meet)
        for t in (2, 1):
            left_copy(t, c).start()

        @pl.when(target != core)
        def _():
            left_copy(0, c).start()

    with scope("right"):
        loads[pieces + 2].wait()
        ready, scales = (jnp.concatenate(list_of, axis=0) for list_of in (ready, scales))
        right = (dot(ready, right_w_ref[...]) * scales).astype(jnp.bfloat16)
        rboth[core] = right

    right_copy = pltpu.make_async_remote_copy(
        src_ref=rboth.at[core],
        dst_ref=rboth.at[core],
        send_sem=rsend_sem,
        recv_sem=rrecv_sem,
        device_id=device(z, 1 - core, second),
        device_id_type=MESH,
    )
    right_copy.start()
    with scope("across"):
        @pl.when(side == 0)
        def _():
            pl.semaphore_wait(across_sem, 1)

        for c in range(pieces):
            left_copy(3, c).start()
    with scope("gate"):
        loads[pieces + 3].wait()
        gates = jax.nn.sigmoid(dot(ready, gate_w_ref[...]) * scales)
        for c in range(pieces):
            for k in range(rows):
                at = c * lump + k * PIECE
                gate[k * cols + c * PIECE : k * cols + (c + 1) * PIECE, :] = gates[at : at + PIECE, :]
        loads[pieces + 4].wait()
        loads[pieces + 5].wait()

    with scope("rwait"):
        right_copy.wait_recv()
    with scope("r32"):
        for q in range(2):
            right32[q] = rboth[q].astype(jnp.float32)

    def send(j, n, slot, to):
        return pltpu.make_async_remote_copy(
            src_ref=psend.at[j, n],
            dst_ref=inbox.at[slot],
            send_sem=psend_sem.at[j, n],
            recv_sem=inbox_sem.at[slot],
            device_id=to,
            device_id_type=MESH,
        )

    near_at, cross_at, own_at = 2 * chunks, 2 * chunks + per_core, 2 * chunks + 2 * per_core
    near_early = jnp.logical_and(upper == side, parity != lax.rem(z, 2))
    held_back = jnp.logical_and(outer, jnp.logical_not(near_early))

    def relay_copy(j, n):
        return send(j, n, j * chunks + n, device(near_z, 1, second))

    def near_copy(j, n):
        return send(j, n, near_at + n % per_core, device(near_z, n // per_core, second))

    def cross_copy(j, n):
        return send(j, n, cross_at + n % per_core, device(planes_of[j], n // per_core, second))

    def own_copy(j, n):
        return send(j, n, own_at + n % per_core, device(z, 1, second))

    def block(j, c):
        with scope(f"wl{j}{c}"):
            for q in range(2):
                mine = jnp.logical_and(from_own, core == q) if j == 0 else None

                def arrived():
                    pltpu.make_async_remote_copy(
                        src_ref=lsend.at[c],
                        dst_ref=lrecv.at[j, q, c],
                        send_sem=lsend_sem.at[0, c],
                        recv_sem=lrecv_sem.at[j, q, c],
                        device_id=device(z, 1 - core, second),
                        device_id_type=MESH,
                    ).wait_recv()
                    left32[c, q] = lrecv[j, q, c].astype(jnp.float32)

                if j:
                    arrived()
                else:
                    pl.when(jnp.logical_not(mine))(arrived)

                    @pl.when(mine)
                    def _():
                        left32[c, q] = lsend[c].astype(jnp.float32)

        with scope(f"block{j}{c}"):
            for part in range(per_piece):
                n = c * per_piece + part
                sums = tuple(jnp.zeros((cols, x_ref.shape[-1]), jnp.float32) for _ in range(CHUNK))
                for q in range(2):

                    def body(k, sums):
                        at = pl.multiple_of(k * PIECE, PIECE)
                        r = jnp.concatenate(
                            [right32[q, pl.ds(p * lump + at, PIECE), :] for p in range(pieces)], axis=0
                        )
                        return tuple(
                            total + left32[c, q, pl.ds(at + part * CHUNK + i, 1), :] * r
                            for i, total in enumerate(sums)
                        )

                    sums = lax.fori_loop(0, rows, body, sums, unroll=True)
                total = jnp.concatenate(sums, axis=0)

                @pl.when(jnp.logical_and(crossing, inner))
                def _():
                    part32[j, n] = total

                psend[j, n] = total.astype(jnp.bfloat16)

                @pl.when(jnp.logical_and(crossing, outer))
                def _():
                    relay_copy(j, n).start()

                @pl.when(is_own[j])
                def _():
                    if n < per_core:
                        inbox[own_at + n] = psend[j, n]
                    else:
                        own_copy(j, n).start()

                @pl.when(jnp.logical_and(is_near[j], jnp.logical_not(held_back)))
                def _():
                    near_copy(j, n).start()

    with scope("nearbar"):

        @pl.when(jnp.logical_and(even, level))
        def _():
            pl.semaphore_wait(near_sem, 2)

        @pl.when(jnp.logical_and(z == 0, crossing))
        def _():
            pl.semaphore_wait(near_sem, 1)

    for j in range(2):
        for c in range(pieces):
            block(j, c)

    by_plane = [(j, n) for j in range(2) for n in range(chunks)]
    with scope("relay"):

        @pl.when(early)
        def _():
            pl.semaphore_wait(cross_sem, 2 * half)

        @pl.when(jnp.logical_and(crossing, inner))
        def _():
            for j, n in by_plane:
                relay_copy(j, n).wait_recv()
                total = part32[j, n] + inbox[j * chunks + n].astype(jnp.float32)
                psend[j, n] = total.astype(jnp.bfloat16)
                cross_copy(j, n).start()

    first_sends, last_sends = by_plane[: -chunks // 2], by_plane[-chunks // 2 :]
    with scope("held"):

        @pl.when(held_back)
        def _():
            @pl.when(crossing)
            def _():
                for j, n in first_sends:
                    relay_copy(j, n).wait_send()
                pl.semaphore_signal(go_sem, inc=1, device_id=device(z, 0, second), device_id_type=MESH)

            @pl.when(level)
            def _():
                pl.semaphore_wait(go_sem, 1)
                for j in range(2):

                    @pl.when(is_near[j])
                    def _():
                        for n in range(chunks):
                            near_copy(j, n).start()

    count = rows * 2 * planes
    for c in range(per_core):
        with scope(f"own{c}"):

            @pl.when(crossing)
            def _():
                own_copy(0, c).wait_recv()

        with scope(f"near{c}"):
            near_copy(0, c).wait_recv()
    with scope("sum"):
        for c in range(per_core):
            part32[0, c] = inbox[own_at + c].astype(jnp.float32) + inbox[near_at + c].astype(jnp.float32)
    with scope("cross"):
        for c in range(per_core):
            cross_copy(0, c).wait_recv()
    with scope("final"):
        total = jnp.concatenate(
            [part32[0, c] + inbox[cross_at + c].astype(jnp.float32) for c in range(per_core)], axis=0
        )
        mixed = (total * count ** (-0.5)).astype(jnp.bfloat16)
        scaled, scale = centre(mixed.astype(jnp.float32), mid_gain_ref[...])
        out_ref[...] = (dot(scaled, out_w_ref[...]) * (gate[...] * scale)).astype(jnp.bfloat16)

    with scope("drain"):
        for t in (1, 2, 3):
            for c in range(pieces):
                left_copy(t, c).wait_send()

        @pl.when(target != core)
        def _():
            for c in range(pieces):
                left_copy(0, c).wait_send()

        right_copy.wait_send()

        @pl.when(crossing)
        def _():
            for j, n in last_sends:
                relay_copy(j, n).wait_send()

            @pl.when(jnp.logical_not(held_back))
            def _():
                for j, n in first_sends:
                    relay_copy(j, n).wait_send()

        @pl.when(level)
        def _():
            for j, n in by_plane:
                if n < per_core:

                    @pl.when(is_near[j])
                    def _():
                        near_copy(j, n).wait_send()

                else:
                    near_copy(j, n).wait_send()


def triangle(planes, lines, pair_rows, in_gain, left_weight, right_weight, mid_gain, out_weight, out_gate):
    rows, cols, width = pair_rows.shape
    mix = left_weight.shape[1]
    pairs, pieces, chunks, size = rows * cols, cols // PIECE, cols // CHUNK, CHUNK * cols
    lump = rows * PIECE
    slots = 2 * chunks + 3 * (chunks // 2)
    anywhere = pl.BlockSpec(memory_space=pl.ANY)
    bf16, f32 = jnp.bfloat16, jnp.float32
    out = pl.pallas_call(
        functools.partial(triangle_kernel, rows, cols, planes, lines),
        out_shape=pltpu.VMEM((pairs, width), bf16),
        in_specs=[anywhere] * 7,
        out_specs=pl.BlockSpec(memory_space=pltpu.VMEM),
        scratch_shapes=[
            pltpu.VMEM((pieces, rows, PIECE, width), bf16),
            pltpu.VMEM((1, width), f32),
            pltpu.VMEM((width, mix), bf16),
            pltpu.VMEM((width, mix), bf16),
            pltpu.VMEM((1, mix), f32),
            pltpu.VMEM((mix, width), bf16),
            pltpu.VMEM((width, width), bf16),
            pltpu.VMEM((pieces, lump, mix), bf16),
            pltpu.VMEM((2, 2, pieces, lump, mix), bf16),
            pltpu.VMEM((2, pairs, mix), bf16),
            pltpu.VMEM((pieces, 2, lump, mix), f32),
            pltpu.VMEM((2, pairs, mix), f32),
            pltpu.VMEM((2, chunks, size, mix), bf16),
            pltpu.VMEM((2, chunks, size, mix), f32),
            pltpu.VMEM((slots, size, mix), bf16),
            pltpu.VMEM((pairs, width), f32),
        ],
        compiler_params=pltpu.CompilerParams(collective_id=0, has_side_effects=True),
    )(
        pair_rows, in_gain.reshape(1, width), left_weight, right_weight,
        mid_gain.reshape(1, mix), out_weight, out_gate,
    )
    return out.reshape(rows, cols, width)


def shards(pair_rows, in_gain, left_weight, right_weight, mid_gain, out_weight, out_gate):
    ready = norm_channels(pair_rows.astype(jnp.float32), in_gain).astype(jnp.bfloat16)
    ready = lax.optimization_barrier(ready)
    left = jnp.einsum("ijc,cd->ijd", ready, left_weight, preferred_element_type=jnp.float32)
    right = jnp.einsum("ijc,cd->ijd", ready, right_weight, preferred_element_type=jnp.float32)
    left, right = left.astype(jnp.bfloat16), right.astype(jnp.bfloat16)
    count = pair_rows.shape[0] * lax.axis_size("first")
    left_lines, right_lines = (
        lax.all_to_all(left, "first", split_axis=2, concat_axis=0, tiled=True),
        lax.all_to_all(right, "first", split_axis=2, concat_axis=0, tiled=True),
    )
    strip = jnp.einsum(
        "kid,kjd->ijd",
        lax.all_gather(left_lines, "second", axis=1, tiled=True),
        right_lines,
        preferred_element_type=jnp.float32,
    )
    strip = (strip * count ** (-0.5)).astype(jnp.bfloat16)
    mixed = lax.all_to_all(strip, "first", split_axis=0, concat_axis=2, tiled=True)
    scaled = norm_channels(mixed.astype(jnp.float32), mid_gain).astype(jnp.bfloat16)
    scaled = lax.optimization_barrier(scaled)
    gate = jax.nn.sigmoid(
        jnp.einsum("ijc,cd->ijd", ready, out_gate, preferred_element_type=jnp.float32)
    )
    return (
        jnp.einsum("ijd,dc->ijc", scaled, out_weight, preferred_element_type=jnp.float32) * gate
    ).astype(jnp.bfloat16)


def solution(mesh):
    in_specs = (P("first", "second", None), P(), P(), P(), P(), P(), P())
    out_specs = P("first", "second", None)
    planes, lines = mesh.shape["first"] // 2, mesh.shape["second"]
    if planes == lines == 4:
        body = functools.partial(triangle, planes, lines)
    else:
        body = shards
    return jax.shard_map(body, mesh=mesh, in_specs=in_specs, out_specs=out_specs, check_vma=False)
```

```python
import functools

import jax
import jax.numpy as jnp
from jax import lax
from jax.experimental import pallas as pl
from jax.experimental.pallas import tpu as pltpu
from jax.sharding import PartitionSpec as P

MESH = pl.DeviceIdType.MESH


def norm_channels(values, channel_gain):
    centred = values - jnp.mean(values, axis=-1, keepdims=True)
    return (
        centred
        * lax.rsqrt(jnp.mean(centred * centred, axis=-1, keepdims=True) + 1e-05)
        * channel_gain
    )


def dot(a, b):
    return jnp.dot(a, b, preferred_element_type=jnp.float32)


PIECE = 8
CHUNK = 4


def other(index):
    return index + 1 - 2 * lax.rem(index, 2)


def centre(values, channel_gain):
    centred = values - jnp.mean(values, axis=-1, keepdims=True)
    scale = lax.rsqrt(jnp.mean(centred * centred, axis=-1, keepdims=True) + 1e-05)
    return (centred * channel_gain).astype(jnp.bfloat16), scale


def triangle_kernel(rows, cols, planes, lines, *refs):
    pieces, chunks = cols // PIECE, cols // CHUNK
    pl.run_scoped(
        functools.partial(triangle_steps, rows, cols, planes, lines, *refs),
        pltpu.SemaphoreType.DMA((6 + pieces,)),
        pltpu.SemaphoreType.DMA((lines, pieces)),
        pltpu.SemaphoreType.DMA((2, 2, pieces)),
        pltpu.SemaphoreType.DMA,
        pltpu.SemaphoreType.DMA,
        pltpu.SemaphoreType.DMA((2, chunks)),
        pltpu.SemaphoreType.DMA((2 * chunks + 3 * (chunks // 2),)),
        pltpu.SemaphoreType.REGULAR,
        pltpu.SemaphoreType.REGULAR,
        pltpu.SemaphoreType.REGULAR,
        pltpu.SemaphoreType.REGULAR,
    )


def triangle_steps(
    rows, cols, planes, lines,
    x_hbm, in_gain_hbm, left_w_hbm, right_w_hbm, mid_gain_hbm, out_w_hbm, gate_w_hbm,
    out_ref,
    x_ref, in_gain_ref, left_w_ref, right_w_ref, mid_gain_ref, out_w_ref, gate_w_ref,
    lsend, lrecv, rboth, left32, right32, psend, part32, inbox, gate,
    in_sem, lsend_sem, lrecv_sem, rsend_sem, rrecv_sem, psend_sem, inbox_sem, go_sem, across_sem, cross_sem, near_sem,
):
    first, second = lax.axis_index("first"), lax.axis_index("second")
    z, core = lax.div(first, 2), lax.rem(first, 2)
    pieces, chunks = cols // PIECE, cols // CHUNK
    per_piece, per_core = PIECE // CHUNK, chunks // 2
    lump, size = rows * PIECE, CHUNK * cols
    half = planes // 2
    upper, side, parity = lax.div(z, half), lax.div(second, half), lax.rem(second, 2)
    near_z = other(z)
    inner = lax.rem(z, 2) != upper
    outer = jnp.logical_not(inner)
    crossing = core == 1
    level = core == 0
    target_side = jnp.where(crossing, 1 - upper, upper)
    planes_of = [half * target_side + lax.rem(parity + u, 2) for u in range(2)]
    from_own = target_side == side
    is_own = [jnp.logical_and(level, planes_of[u] == z) for u in range(2)]
    is_near = [jnp.logical_and(level, planes_of[u] != z) for u in range(2)]
    x_second, y_second = other(second), lax.rem(second + half, lines)
    xy_second = other(y_second)
    cross_z = 2 * lax.rem(upper + 1, 2) + lax.rem(upper + 1 + 1, 2)

    def device(z_at, core_at, second_at):
        return {"first": 2 * z_at + core_at, "second": second_at}

    scope = jax.named_scope
    barrier = pltpu.get_barrier_semaphore()

    def greet(z_at, core_at, second_at):
        pl.semaphore_signal(
            barrier, inc=1, device_id=device(z_at, core_at, second_at), device_id_type=MESH
        )

    target = lax.rem(side + upper, 2)
    early = jnp.logical_and(crossing, jnp.logical_and(inner, upper == 0))
    even = lax.rem(z, 2) == 0
    last_column = second == lines - 1
    slow_column = second == half

    with scope("sig"):
        greet(z, 1 - core, second)
        for c in range(2):

            @pl.when(from_own)
            def _():
                greet(z, c, x_second)

            @pl.when(jnp.logical_not(from_own))
            def _():
                greet(z, c, y_second)

        @pl.when(side == 0)
        def _():
            greet(z, target, xy_second)

            @pl.when(jnp.logical_not(from_own))
            def _():
                for c in range(2):
                    greet(z, c, xy_second)

        @pl.when(even)
        def _():
            greet(near_z, 0, second)

            @pl.when(level)
            def _():
                for c in range(2):
                    greet(near_z, c, second)

            @pl.when(crossing)
            def _():
                greet(near_z, 1, second)

        @pl.when(upper == 0)
        def _():
            greet(cross_z, 1, second)

        @pl.when(early)
        def _():
            for dz in range(half):
                for c in range(2):
                    greet(half + dz, c, second)

    loads = [
        pltpu.make_async_copy(src, dst, in_sem.at[n])
        for n, (src, dst) in enumerate((
            (in_gain_hbm, in_gain_ref), (left_w_hbm, left_w_ref),
            *((x_hbm.at[:, pl.ds(c * PIECE, PIECE), :], x_ref.at[c]) for c in range(pieces)),
            (right_w_hbm, right_w_ref),
            (gate_w_hbm, gate_w_ref), (mid_gain_hbm, mid_gain_ref), (out_w_hbm, out_w_ref),
        ))
    ]
    for load in loads:
        load.start()
    def meet():
        signals = (
            3
            + jnp.where(even, 0, 1 + jnp.where(level, 2, 1))
            + jnp.where(jnp.logical_and(crossing, z == half), 2 * half, 0)
            + jnp.where(side == 0, 0, 1 + jnp.where(from_own, 0, 2))
            + upper
        )
        pl.semaphore_wait(barrier, signals.astype(jnp.int32))

        def answer(semaphore, z_at, core_at, second_at):
            pl.semaphore_signal(
                semaphore, inc=1, device_id=device(z_at, core_at, second_at), device_id_type=MESH
            )

        @pl.when(jnp.logical_and(side == 1, jnp.logical_not(from_own)))
        def _():
            for c in range(2):
                answer(across_sem, z, c, xy_second)

        @pl.when(jnp.logical_not(even))
        def _():
            answer(near_sem, near_z, 0, second)

        @pl.when(early)
        def _():
            answer(near_sem, near_z, 1, second)

        @pl.when(upper == 1)
        def _():
            answer(cross_sem, cross_z, 1, second)

    with scope("bar"):
        pl.when(last_column)(meet)

    def left_copy(t, c):
        return pltpu.make_async_remote_copy(
            src_ref=lsend.at[c],
            dst_ref=lrecv.at[t % 2, core, c],
            send_sem=lsend_sem.at[t, c],
            recv_sem=lrecv_sem.at[t % 2, core, c],
            device_id=device(z, target, (second, x_second, y_second, xy_second)[t]),
            device_id_type=MESH,
        )

    with scope("load"):
        loads[0].wait()
        loads[1].wait()

    def send_left(c):
        for t in (2, 1):
            left_copy(t, c).start()

        @pl.when(target != core)
        def _():
            left_copy(0, c).start()

    ready, scales = [], []
    for c in range(pieces):
        with scope(f"left{c}"):
            loads[2 + c].wait()
            x = x_ref[c].astype(jnp.float32).reshape(lump, x_ref.shape[-1])
            for list_of, value in zip((ready, scales), centre(x, in_gain_ref[...])):
                list_of.append(value)
            lsend[c] = (dot(ready[c], left_w_ref[...]) * scales[c]).astype(jnp.bfloat16)
        if c == 0:
            with scope("bar0"):
                pl.when(side == 0)(meet)

        @pl.when(jnp.logical_not(slow_column))
        def _():
            send_left(c)

    with scope("right"):
        loads[pieces + 2].wait()
        ready, scales = (jnp.concatenate(list_of, axis=0) for list_of in (ready, scales))
        right = (dot(ready, right_w_ref[...]) * scales).astype(jnp.bfloat16)
        rboth[core] = right
    with scope("bar2"):

        @pl.when(slow_column)
        def _():
            meet()
            for c in range(pieces):
                send_left(c)

    right_copy = pltpu.make_async_remote_copy(
        src_ref=rboth.at[core],
        dst_ref=rboth.at[core],
        send_sem=rsend_sem,
        recv_sem=rrecv_sem,
        device_id=device(z, 1 - core, second),
        device_id_type=MESH,
    )
    right_copy.start()
    with scope("across"):
        @pl.when(side == 0)
        def _():
            pl.semaphore_wait(across_sem, 1)

        for c in range(pieces):
            left_copy(3, c).start()
    with scope("gate"):
        loads[pieces + 3].wait()
        gates = jax.nn.sigmoid(dot(ready, gate_w_ref[...]) * scales)
        for c in range(pieces):
            for k in range(rows):
                at = c * lump + k * PIECE
                gate[k * cols + c * PIECE : k * cols + (c + 1) * PIECE, :] = gates[at : at + PIECE, :]
        loads[pieces + 4].wait()
        loads[pieces + 5].wait()

    with scope("rwait"):
        right_copy.wait_recv()
    with scope("r32"):
        for q in range(2):
            right32[q] = rboth[q].astype(jnp.float32)

    def send(j, n, slot, to):
        return pltpu.make_async_remote_copy(
            src_ref=psend.at[j, n],
            dst_ref=inbox.at[slot],
            send_sem=psend_sem.at[j, n],
            recv_sem=inbox_sem.at[slot],
            device_id=to,
            device_id_type=MESH,
        )

    near_at, cross_at, own_at = 2 * chunks, 2 * chunks + per_core, 2 * chunks + 2 * per_core
    near_early = jnp.logical_and(upper == side, parity != lax.rem(z, 2))
    held_back = jnp.logical_and(outer, jnp.logical_not(near_early))

    def relay_copy(j, n):
        return send(j, n, j * chunks + n, device(near_z, 1, second))

    def near_copy(j, n):
        return send(j, n, near_at + n % per_core, device(near_z, n // per_core, second))

    def cross_copy(j, n):
        return send(j, n, cross_at + n % per_core, device(planes_of[j], n // per_core, second))

    def own_copy(j, n):
        return send(j, n, own_at + n % per_core, device(z, 1, second))

    def block(j, c):
        with scope(f"wl{j}{c}"):
            for q in range(2):
                mine = jnp.logical_and(from_own, core == q) if j == 0 else None

                def arrived():
                    pltpu.make_async_remote_copy(
                        src_ref=lsend.at[c],
                        dst_ref=lrecv.at[j, q, c],
                        send_sem=lsend_sem.at[0, c],
                        recv_sem=lrecv_sem.at[j, q, c],
                        device_id=device(z, 1 - core, second),
                        device_id_type=MESH,
                    ).wait_recv()
                    left32[c, q] = lrecv[j, q, c].astype(jnp.float32)

                if j:
                    arrived()
                else:
                    pl.when(jnp.logical_not(mine))(arrived)

                    @pl.when(mine)
                    def _():
                        left32[c, q] = lsend[c].astype(jnp.float32)

        with scope(f"block{j}{c}"):
            for part in range(per_piece):
                n = c * per_piece + part
                sums = tuple(jnp.zeros((cols, x_ref.shape[-1]), jnp.float32) for _ in range(CHUNK))
                for q in range(2):

                    def body(k, sums):
                        at = pl.multiple_of(k * PIECE, PIECE)
                        r = jnp.concatenate(
                            [right32[q, pl.ds(p * lump + at, PIECE), :] for p in range(pieces)], axis=0
                        )
                        return tuple(
                            total + left32[c, q, pl.ds(at + part * CHUNK + i, 1), :] * r
                            for i, total in enumerate(sums)
                        )

                    sums = lax.fori_loop(0, rows, body, sums, unroll=True)
                total = jnp.concatenate(sums, axis=0)

                @pl.when(jnp.logical_and(crossing, inner))
                def _():
                    part32[j, n] = total

                psend[j, n] = total.astype(jnp.bfloat16)

                @pl.when(jnp.logical_and(crossing, outer))
                def _():
                    relay_copy(j, n).start()

                @pl.when(is_own[j])
                def _():
                    if n < per_core:
                        inbox[own_at + n] = psend[j, n]
                    else:
                        own_copy(j, n).start()

                @pl.when(jnp.logical_and(is_near[j], jnp.logical_not(held_back)))
                def _():
                    near_copy(j, n).start()

    with scope("nearbar"):

        @pl.when(jnp.logical_and(even, level))
        def _():
            pl.semaphore_wait(near_sem, 2)

        @pl.when(jnp.logical_and(z == 0, crossing))
        def _():
            pl.semaphore_wait(near_sem, 1)

    for j in range(2):
        for c in range(pieces):
            block(j, c)

    by_plane = [(j, n) for j in range(2) for n in range(chunks)]
    with scope("relay"):

        @pl.when(early)
        def _():
            pl.semaphore_wait(cross_sem, 2 * half)

        @pl.when(jnp.logical_and(crossing, inner))
        def _():
            for j, n in by_plane:
                relay_copy(j, n).wait_recv()
                total = part32[j, n] + inbox[j * chunks + n].astype(jnp.float32)
                psend[j, n] = total.astype(jnp.bfloat16)
                cross_copy(j, n).start()

    first_sends, last_sends = by_plane[: -chunks // 2], by_plane[-chunks // 2 :]
    with scope("held"):

        @pl.when(held_back)
        def _():
            @pl.when(crossing)
            def _():
                for j, n in first_sends:
                    relay_copy(j, n).wait_send()
                pl.semaphore_signal(go_sem, inc=1, device_id=device(z, 0, second), device_id_type=MESH)

            @pl.when(level)
            def _():
                pl.semaphore_wait(go_sem, 1)
                for j in range(2):

                    @pl.when(is_near[j])
                    def _():
                        for n in range(chunks):
                            near_copy(j, n).start()

    count = rows * 2 * planes
    for c in range(per_core):
        with scope(f"own{c}"):

            @pl.when(crossing)
            def _():
                own_copy(0, c).wait_recv()

        with scope(f"near{c}"):
            near_copy(0, c).wait_recv()
    with scope("sum"):
        for c in range(per_core):
            part32[0, c] = inbox[own_at + c].astype(jnp.float32) + inbox[near_at + c].astype(jnp.float32)
    with scope("cross"):
        for c in range(per_core):
            cross_copy(0, c).wait_recv()
    with scope("final"):
        total = jnp.concatenate(
            [part32[0, c] + inbox[cross_at + c].astype(jnp.float32) for c in range(per_core)], axis=0
        )
        mixed = (total * count ** (-0.5)).astype(jnp.bfloat16)
        scaled, scale = centre(mixed.astype(jnp.float32), mid_gain_ref[...])
        out_ref[...] = (dot(scaled, out_w_ref[...]) * (gate[...] * scale)).astype(jnp.bfloat16)

    with scope("drain"):
        for t in (1, 2, 3):
            for c in range(pieces):
                left_copy(t, c).wait_send()

        @pl.when(target != core)
        def _():
            for c in range(pieces):
                left_copy(0, c).wait_send()

        right_copy.wait_send()

        @pl.when(crossing)
        def _():
            for j, n in last_sends:
                relay_copy(j, n).wait_send()

            @pl.when(jnp.logical_not(held_back))
            def _():
                for j, n in first_sends:
                    relay_copy(j, n).wait_send()

        @pl.when(level)
        def _():
            for j, n in by_plane:
                if n < per_core:

                    @pl.when(is_near[j])
                    def _():
                        near_copy(j, n).wait_send()

                else:
                    near_copy(j, n).wait_send()


def triangle(planes, lines, pair_rows, in_gain, left_weight, right_weight, mid_gain, out_weight, out_gate):
    rows, cols, width = pair_rows.shape
    mix = left_weight.shape[1]
    pairs, pieces, chunks, size = rows * cols, cols // PIECE, cols // CHUNK, CHUNK * cols
    lump = rows * PIECE
    slots = 2 * chunks + 3 * (chunks // 2)
    anywhere = pl.BlockSpec(memory_space=pl.ANY)
    bf16, f32 = jnp.bfloat16, jnp.float32
    out = pl.pallas_call(
        functools.partial(triangle_kernel, rows, cols, planes, lines),
        out_shape=pltpu.VMEM((pairs, width), bf16),
        in_specs=[anywhere] * 7,
        out_specs=pl.BlockSpec(memory_space=pltpu.VMEM),
        scratch_shapes=[
            pltpu.VMEM((pieces, rows, PIECE, width), bf16),
            pltpu.VMEM((1, width), f32),
            pltpu.VMEM((width, mix), bf16),
            pltpu.VMEM((width, mix), bf16),
            pltpu.VMEM((1, mix), f32),
            pltpu.VMEM((mix, width), bf16),
            pltpu.VMEM((width, width), bf16),
            pltpu.VMEM((pieces, lump, mix), bf16),
            pltpu.VMEM((2, 2, pieces, lump, mix), bf16),
            pltpu.VMEM((2, pairs, mix), bf16),
            pltpu.VMEM((pieces, 2, lump, mix), f32),
            pltpu.VMEM((2, pairs, mix), f32),
            pltpu.VMEM((2, chunks, size, mix), bf16),
            pltpu.VMEM((2, chunks, size, mix), f32),
            pltpu.VMEM((slots, size, mix), bf16),
            pltpu.VMEM((pairs, width), f32),
        ],
        compiler_params=pltpu.CompilerParams(collective_id=0, has_side_effects=True),
    )(
        pair_rows, in_gain.reshape(1, width), left_weight, right_weight,
        mid_gain.reshape(1, mix), out_weight, out_gate,
    )
    return out.reshape(rows, cols, width)


def shards(pair_rows, in_gain, left_weight, right_weight, mid_gain, out_weight, out_gate):
    ready = norm_channels(pair_rows.astype(jnp.float32), in_gain).astype(jnp.bfloat16)
    ready = lax.optimization_barrier(ready)
    left = jnp.einsum("ijc,cd->ijd", ready, left_weight, preferred_element_type=jnp.float32)
    right = jnp.einsum("ijc,cd->ijd", ready, right_weight, preferred_element_type=jnp.float32)
    left, right = left.astype(jnp.bfloat16), right.astype(jnp.bfloat16)
    count = pair_rows.shape[0] * lax.axis_size("first")
    left_lines, right_lines = (
        lax.all_to_all(left, "first", split_axis=2, concat_axis=0, tiled=True),
        lax.all_to_all(right, "first", split_axis=2, concat_axis=0, tiled=True),
    )
    strip = jnp.einsum(
        "kid,kjd->ijd",
        lax.all_gather(left_lines, "second", axis=1, tiled=True),
        right_lines,
        preferred_element_type=jnp.float32,
    )
    strip = (strip * count ** (-0.5)).astype(jnp.bfloat16)
    mixed = lax.all_to_all(strip, "first", split_axis=0, concat_axis=2, tiled=True)
    scaled = norm_channels(mixed.astype(jnp.float32), mid_gain).astype(jnp.bfloat16)
    scaled = lax.optimization_barrier(scaled)
    gate = jax.nn.sigmoid(
        jnp.einsum("ijc,cd->ijd", ready, out_gate, preferred_element_type=jnp.float32)
    )
    return (
        jnp.einsum("ijd,dc->ijc", scaled, out_weight, preferred_element_type=jnp.float32) * gate
    ).astype(jnp.bfloat16)


def solution(mesh):
    in_specs = (P("first", "second", None), P(), P(), P(), P(), P(), P())
    out_specs = P("first", "second", None)
    planes, lines = mesh.shape["first"] // 2, mesh.shape["second"]
    if planes == lines == 4:
        body = functools.partial(triangle, planes, lines)
    else:
        body = shards
    return jax.shard_map(body, mesh=mesh, in_specs=in_specs, out_specs=out_specs, check_vma=False)
```

```python
import functools

import jax
import jax.numpy as jnp
from jax import lax
from jax.experimental import pallas as pl
from jax.experimental.pallas import tpu as pltpu
from jax.sharding import PartitionSpec as P

MESH = pl.DeviceIdType.MESH


def norm_channels(values, channel_gain):
    centred = values - jnp.mean(values, axis=-1, keepdims=True)
    return (
        centred
        * lax.rsqrt(jnp.mean(centred * centred, axis=-1, keepdims=True) + 1e-05)
        * channel_gain
    )


def dot(a, b):
    return jnp.dot(a, b, preferred_element_type=jnp.float32)


PIECE = 8
CHUNK = 2
DIRECT = 2


def other(index):
    return index + 1 - 2 * lax.rem(index, 2)


def centre(values, channel_gain):
    centred = values - jnp.mean(values, axis=-1, keepdims=True)
    scale = lax.rsqrt(jnp.mean(centred * centred, axis=-1, keepdims=True) + 1e-05)
    return (centred * channel_gain).astype(jnp.bfloat16), scale


def triangle_kernel(rows, cols, planes, lines, *refs):
    pieces, chunks = cols // PIECE, cols // CHUNK
    pl.run_scoped(
        functools.partial(triangle_steps, rows, cols, planes, lines, *refs),
        pltpu.SemaphoreType.DMA((6 + pieces,)),
        pltpu.SemaphoreType.DMA((lines, pieces)),
        pltpu.SemaphoreType.DMA((2, 2, pieces)),
        pltpu.SemaphoreType.DMA,
        pltpu.SemaphoreType.DMA,
        pltpu.SemaphoreType.DMA((2, chunks)),
        pltpu.SemaphoreType.DMA((2 * chunks + 4 * (chunks // 2),)),
        pltpu.SemaphoreType.REGULAR,
        pltpu.SemaphoreType.REGULAR,
        pltpu.SemaphoreType.REGULAR,
        pltpu.SemaphoreType.REGULAR,
    )


def triangle_steps(
    rows, cols, planes, lines,
    x_hbm, in_gain_hbm, left_w_hbm, right_w_hbm, mid_gain_hbm, out_w_hbm, gate_w_hbm,
    out_ref,
    x_ref, in_gain_ref, left_w_ref, right_w_ref, mid_gain_ref, out_w_ref, gate_w_ref,
    lsend, lrecv, rboth, left32, right32, psend, part32, inbox, gate,
    in_sem, lsend_sem, lrecv_sem, rsend_sem, rrecv_sem, psend_sem, inbox_sem, go_sem, across_sem, cross_sem, near_sem,
):
    first, second = lax.axis_index("first"), lax.axis_index("second")
    z, core = lax.div(first, 2), lax.rem(first, 2)
    pieces, chunks = cols // PIECE, cols // CHUNK
    per_piece, per_core = PIECE // CHUNK, chunks // 2
    lump, size = rows * PIECE, CHUNK * cols
    half = planes // 2
    upper, side, parity = lax.div(z, half), lax.div(second, half), lax.rem(second, 2)
    near_z = other(z)
    inner = lax.rem(z, 2) != upper
    outer = jnp.logical_not(inner)
    crossing = core == 1
    level = core == 0
    target_side = jnp.where(crossing, 1 - upper, upper)
    planes_of = [half * target_side + lax.rem(parity + u, 2) for u in range(2)]
    from_own = target_side == side
    is_own = [jnp.logical_and(level, planes_of[u] == z) for u in range(2)]
    is_near = [jnp.logical_and(level, planes_of[u] != z) for u in range(2)]
    x_second, y_second = other(second), lax.rem(second + half, lines)
    xy_second = other(y_second)
    cross_z = 2 * lax.rem(upper + 1, 2) + lax.rem(upper + 1 + 1, 2)

    def device(z_at, core_at, second_at):
        return {"first": 2 * z_at + core_at, "second": second_at}

    scope = jax.named_scope
    barrier = pltpu.get_barrier_semaphore()

    def greet(z_at, core_at, second_at):
        pl.semaphore_signal(
            barrier, inc=1, device_id=device(z_at, core_at, second_at), device_id_type=MESH
        )

    target = lax.rem(side + upper, 2)
    early = jnp.logical_and(crossing, jnp.logical_and(inner, upper == 0))
    even = lax.rem(z, 2) == 0
    far_target = jnp.logical_and(jnp.logical_and(crossing, upper == 0), lax.rem(z, 2) != parity)
    last_column = second == lines - 1
    slow_column = second == half

    with scope("sig"):
        greet(z, 1 - core, second)

        @pl.when(far_target)
        def _():
            greet(planes - 1, 1, second)

        for c in range(2):

            @pl.when(from_own)
            def _():
                greet(z, c, x_second)

            @pl.when(jnp.logical_not(from_own))
            def _():
                greet(z, c, y_second)

        @pl.when(side == 0)
        def _():
            greet(z, core, jnp.where(parity == 0, x_second, xy_second))

            @pl.when(jnp.logical_not(from_own))
            def _():
                for c in range(2):
                    greet(z, c, xy_second)

        @pl.when(even)
        def _():
            greet(near_z, 0, second)

            @pl.when(level)
            def _():
                for c in range(2):
                    greet(near_z, c, second)

            @pl.when(crossing)
            def _():
                greet(near_z, 1, second)

        @pl.when(upper == 0)
        def _():
            greet(cross_z, 1, second)

        @pl.when(early)
        def _():
            for dz in range(half):
                for c in range(2):
                    greet(half + dz, c, second)

    loads = [
        pltpu.make_async_copy(src, dst, in_sem.at[n])
        for n, (src, dst) in enumerate((
            (in_gain_hbm, in_gain_ref), (left_w_hbm, left_w_ref),
            *((x_hbm.at[:, pl.ds(c * PIECE, PIECE), :], x_ref.at[c]) for c in range(pieces)),
            (right_w_hbm, right_w_ref),
            (gate_w_hbm, gate_w_ref), (mid_gain_hbm, mid_gain_ref), (out_w_hbm, out_w_ref),
        ))
    ]
    for load in loads:
        load.start()
    def meet():
        signals = (
            3
            + jnp.where(even, 0, 1 + jnp.where(level, 2, 1))
            + jnp.where(jnp.logical_and(crossing, z == half), 2 * half, 0)
            + jnp.where(jnp.logical_and(crossing, z == planes - 1), 1, 0)
            + jnp.where(side == 0, parity, 2 - parity)
            + upper
        )
        pl.semaphore_wait(barrier, signals.astype(jnp.int32))

        def answer(semaphore, z_at, core_at, second_at):
            pl.semaphore_signal(
                semaphore, inc=1, device_id=device(z_at, core_at, second_at), device_id_type=MESH
            )

        @pl.when(slow_column)
        def _():
            answer(across_sem, z, core, xy_second)

        @pl.when(jnp.logical_and(side == 0, parity == 1))
        def _():
            answer(across_sem, z, core, x_second)

        @pl.when(jnp.logical_not(even))
        def _():
            answer(near_sem, near_z, 0, second)

        @pl.when(early)
        def _():
            answer(near_sem, near_z, 1, second)

        @pl.when(upper == 1)
        def _():
            answer(cross_sem, cross_z, 1, second)

    with scope("bar"):
        pl.when(last_column)(meet)

    def left_copy(t, c):
        return pltpu.make_async_remote_copy(
            src_ref=lsend.at[c],
            dst_ref=lrecv.at[t % 2, core, c],
            send_sem=lsend_sem.at[t, c],
            recv_sem=lrecv_sem.at[t % 2, core, c],
            device_id=device(z, target, (second, x_second, y_second, xy_second)[t]),
            device_id_type=MESH,
        )

    with scope("load"):
        loads[0].wait()
        loads[1].wait()

    def send_left(c):
        for t in (2, 1):
            left_copy(t, c).start()

        @pl.when(target != core)
        def _():
            left_copy(0, c).start()

    ready, scales = [], []
    for c in range(pieces):
        with scope(f"left{c}"):
            loads[2 + c].wait()
            x = x_ref[c].astype(jnp.float32).reshape(lump, x_ref.shape[-1])
            for list_of, value in zip((ready, scales), centre(x, in_gain_ref[...])):
                list_of.append(value)
            lsend[c] = (dot(ready[c], left_w_ref[...]) * scales[c]).astype(jnp.bfloat16)
        if c == 0:
            with scope("bar0"):
                pl.when(side == 0)(meet)

        @pl.when(jnp.logical_not(slow_column))
        def _():
            send_left(c)

    with scope("right"):
        loads[pieces + 2].wait()
        ready, scales = (jnp.concatenate(list_of, axis=0) for list_of in (ready, scales))
        right = (dot(ready, right_w_ref[...]) * scales).astype(jnp.bfloat16)
        rboth[core] = right
    with scope("bar2"):

        @pl.when(slow_column)
        def _():
            meet()
            for c in range(pieces):
                send_left(c)

    right_copy = pltpu.make_async_remote_copy(
        src_ref=rboth.at[core],
        dst_ref=rboth.at[core],
        send_sem=rsend_sem,
        recv_sem=rrecv_sem,
        device_id=device(z, 1 - core, second),
        device_id_type=MESH,
    )
    right_copy.start()
    with scope("across"):
        @pl.when(side == 0)
        def _():
            pl.semaphore_wait(across_sem, 1)

        for c in range(pieces):
            left_copy(3, c).start()
    with scope("gate"):
        loads[pieces + 3].wait()
        gates = jax.nn.sigmoid(dot(ready, gate_w_ref[...]) * scales)
        for c in range(pieces):
            for k in range(rows):
                at = c * lump + k * PIECE
                gate[k * cols + c * PIECE : k * cols + (c + 1) * PIECE, :] = gates[at : at + PIECE, :]
        loads[pieces + 4].wait()
        loads[pieces + 5].wait()

    with scope("rwait"):
        right_copy.wait_recv()
    with scope("r32"):
        for q in range(2):
            right32[q] = rboth[q].astype(jnp.float32)

    def send(j, n, slot, to):
        return pltpu.make_async_remote_copy(
            src_ref=psend.at[j, n],
            dst_ref=inbox.at[slot],
            send_sem=psend_sem.at[j, n],
            recv_sem=inbox_sem.at[slot],
            device_id=to,
            device_id_type=MESH,
        )

    near_at, cross_at, own_at, far_at = (2 * chunks + n * per_core for n in range(4))
    descending = jnp.logical_and(crossing, upper == 1)

    def skips(j, n):
        return j == 1 and n >= chunks - DIRECT

    near_early = jnp.logical_and(upper == side, parity != lax.rem(z, 2))
    held_back = jnp.logical_and(outer, jnp.logical_not(near_early))

    def relay_copy(j, n):
        return send(j, n, j * chunks + n, device(near_z, 1, second))

    def far_copy(j, n):
        return send(j, n, far_at + n % per_core, device(planes_of[j], 1, second))

    def near_copy(j, n):
        return send(j, n, near_at + n % per_core, device(near_z, n // per_core, second))

    def cross_copy(j, n):
        return send(j, n, cross_at + n % per_core, device(planes_of[j], n // per_core, second))

    def own_copy(j, n):
        return send(j, n, own_at + n % per_core, device(z, 1, second))

    def block(j, c):
        with scope(f"wl{j}{c}"):
            for q in range(2):
                mine = jnp.logical_and(from_own, core == q) if j == 0 else None

                def arrived():
                    pltpu.make_async_remote_copy(
                        src_ref=lsend.at[c],
                        dst_ref=lrecv.at[j, q, c],
                        send_sem=lsend_sem.at[0, c],
                        recv_sem=lrecv_sem.at[j, q, c],
                        device_id=device(z, 1 - core, second),
                        device_id_type=MESH,
                    ).wait_recv()
                    left32[c, q] = lrecv[j, q, c].astype(jnp.float32)

                if j:
                    arrived()
                else:
                    pl.when(jnp.logical_not(mine))(arrived)

                    @pl.when(mine)
                    def _():
                        left32[c, q] = lsend[c].astype(jnp.float32)

        with scope(f"block{j}{c}"):
            for part in range(per_piece):
                n = c * per_piece + part
                sums = tuple(jnp.zeros((cols, x_ref.shape[-1]), jnp.float32) for _ in range(CHUNK))
                for q in range(2):

                    def body(k, sums):
                        at = pl.multiple_of(k * PIECE, PIECE)
                        r = jnp.concatenate(
                            [right32[q, pl.ds(p * lump + at, PIECE), :] for p in range(pieces)], axis=0
                        )
                        return tuple(
                            total + left32[c, q, pl.ds(at + part * CHUNK + i, 1), :] * r
                            for i, total in enumerate(sums)
                        )

                    sums = lax.fori_loop(0, rows, body, sums, unroll=True)
                total = jnp.concatenate(sums, axis=0)

                @pl.when(jnp.logical_and(crossing, inner))
                def _():
                    part32[j, n] = total

                psend[j, n] = total.astype(jnp.bfloat16)

                @pl.when(jnp.logical_and(crossing, jnp.logical_and(outer, upper == 0) if skips(j, n) else outer))
                def _():
                    relay_copy(j, n).start()

                if skips(j, n):

                    @pl.when(jnp.logical_and(descending, outer))
                    def _():
                        far_copy(j, n).start()

                    @pl.when(jnp.logical_and(descending, inner))
                    def _():
                        cross_copy(j, n).start()

                @pl.when(is_own[j])
                def _():
                    if n < per_core:
                        inbox[own_at + n] = psend[j, n]
                    else:
                        own_copy(j, n).start()

                @pl.when(jnp.logical_and(is_near[j], jnp.logical_not(held_back)))
                def _():
                    near_copy(j, n).start()

    with scope("nearbar"):

        @pl.when(jnp.logical_and(even, level))
        def _():
            pl.semaphore_wait(near_sem, 2)

        @pl.when(jnp.logical_and(z == 0, crossing))
        def _():
            pl.semaphore_wait(near_sem, 1)

    for j in range(2):
        for c in range(pieces):
            block(j, c)

    by_plane = [(j, n) for j in range(2) for n in range(chunks)]
    with scope("relay"):

        @pl.when(early)
        def _():
            pl.semaphore_wait(cross_sem, 2 * half)

        @pl.when(jnp.logical_and(crossing, inner))
        def _():
            for j, n in by_plane:

                def relay():
                    relay_copy(j, n).wait_recv()
                    total = part32[j, n] + inbox[j * chunks + n].astype(jnp.float32)
                    psend[j, n] = total.astype(jnp.bfloat16)
                    cross_copy(j, n).start()

                if skips(j, n):
                    pl.when(upper == 0)(relay)
                else:
                    relay()

    first_sends, last_sends = by_plane[: -chunks // 4], by_plane[-chunks // 4 :]
    with scope("held"):

        @pl.when(held_back)
        def _():
            @pl.when(crossing)
            def _():
                for j, n in first_sends:
                    relay_copy(j, n).wait_send()
                pl.semaphore_signal(go_sem, inc=1, device_id=device(z, 0, second), device_id_type=MESH)

            @pl.when(level)
            def _():
                pl.semaphore_wait(go_sem, 1)
                for j in range(2):

                    @pl.when(is_near[j])
                    def _():
                        for n in range(chunks):
                            near_copy(j, n).start()

    count = rows * 2 * planes
    for c in range(per_core):
        with scope(f"own{c}"):

            @pl.when(crossing)
            def _():
                own_copy(0, c).wait_recv()

        with scope(f"near{c}"):
            near_copy(0, c).wait_recv()
    with scope("sum"):
        for c in range(per_core):
            part32[0, c] = inbox[own_at + c].astype(jnp.float32) + inbox[near_at + c].astype(jnp.float32)
    with scope("cross"):
        for c in range(per_core):
            cross_copy(0, c).wait_recv()
    with scope("far"):

        @pl.when(far_target)
        def _():
            for c in range(per_core - DIRECT, per_core):
                part32[0, c] = part32[0, c] + inbox[cross_at + c].astype(jnp.float32)
                send(0, c, far_at + c, device(near_z, 0, second)).wait_recv()

    last_at = [
        (jnp.where(far_target, far_at, cross_at) if c >= per_core - DIRECT else cross_at) + c
        for c in range(per_core)
    ]
    with scope("final"):
        total = jnp.concatenate(
            [part32[0, c] + inbox[last_at[c]].astype(jnp.float32) for c in range(per_core)], axis=0
        )
        mixed = (total * count ** (-0.5)).astype(jnp.bfloat16)
        scaled, scale = centre(mixed.astype(jnp.float32), mid_gain_ref[...])
        out_ref[...] = (dot(scaled, out_w_ref[...]) * (gate[...] * scale)).astype(jnp.bfloat16)

    with scope("drain"):
        for t in (1, 2, 3):
            for c in range(pieces):
                left_copy(t, c).wait_send()

        @pl.when(target != core)
        def _():
            for c in range(pieces):
                left_copy(0, c).wait_send()

        right_copy.wait_send()

        @pl.when(crossing)
        def _():
            for j, n in last_sends:
                relay_copy(j, n).wait_send()

            @pl.when(jnp.logical_not(held_back))
            def _():
                for j, n in first_sends:
                    relay_copy(j, n).wait_send()

        @pl.when(level)
        def _():
            for j, n in by_plane:
                if n < per_core:

                    @pl.when(is_near[j])
                    def _():
                        near_copy(j, n).wait_send()

                else:
                    near_copy(j, n).wait_send()


def triangle(planes, lines, pair_rows, in_gain, left_weight, right_weight, mid_gain, out_weight, out_gate):
    rows, cols, width = pair_rows.shape
    mix = left_weight.shape[1]
    pairs, pieces, chunks, size = rows * cols, cols // PIECE, cols // CHUNK, CHUNK * cols
    lump = rows * PIECE
    slots = 2 * chunks + 4 * (chunks // 2)
    anywhere = pl.BlockSpec(memory_space=pl.ANY)
    bf16, f32 = jnp.bfloat16, jnp.float32
    out = pl.pallas_call(
        functools.partial(triangle_kernel, rows, cols, planes, lines),
        out_shape=pltpu.VMEM((pairs, width), bf16),
        in_specs=[anywhere] * 7,
        out_specs=pl.BlockSpec(memory_space=pltpu.VMEM),
        scratch_shapes=[
            pltpu.VMEM((pieces, rows, PIECE, width), bf16),
            pltpu.VMEM((1, width), f32),
            pltpu.VMEM((width, mix), bf16),
            pltpu.VMEM((width, mix), bf16),
            pltpu.VMEM((1, mix), f32),
            pltpu.VMEM((mix, width), bf16),
            pltpu.VMEM((width, width), bf16),
            pltpu.VMEM((pieces, lump, mix), bf16),
            pltpu.VMEM((2, 2, pieces, lump, mix), bf16),
            pltpu.VMEM((2, pairs, mix), bf16),
            pltpu.VMEM((pieces, 2, lump, mix), f32),
            pltpu.VMEM((2, pairs, mix), f32),
            pltpu.VMEM((2, chunks, size, mix), bf16),
            pltpu.VMEM((2, chunks, size, mix), f32),
            pltpu.VMEM((slots, size, mix), bf16),
            pltpu.VMEM((pairs, width), f32),
        ],
        compiler_params=pltpu.CompilerParams(collective_id=0, has_side_effects=True),
    )(
        pair_rows, in_gain.reshape(1, width), left_weight, right_weight,
        mid_gain.reshape(1, mix), out_weight, out_gate,
    )
    return out.reshape(rows, cols, width)


def shards(pair_rows, in_gain, left_weight, right_weight, mid_gain, out_weight, out_gate):
    ready = norm_channels(pair_rows.astype(jnp.float32), in_gain).astype(jnp.bfloat16)
    ready = lax.optimization_barrier(ready)
    left = jnp.einsum("ijc,cd->ijd", ready, left_weight, preferred_element_type=jnp.float32)
    right = jnp.einsum("ijc,cd->ijd", ready, right_weight, preferred_element_type=jnp.float32)
    left, right = left.astype(jnp.bfloat16), right.astype(jnp.bfloat16)
    count = pair_rows.shape[0] * lax.axis_size("first")
    left_lines, right_lines = (
        lax.all_to_all(left, "first", split_axis=2, concat_axis=0, tiled=True),
        lax.all_to_all(right, "first", split_axis=2, concat_axis=0, tiled=True),
    )
    strip = jnp.einsum(
        "kid,kjd->ijd",
        lax.all_gather(left_lines, "second", axis=1, tiled=True),
        right_lines,
        preferred_element_type=jnp.float32,
    )
    strip = (strip * count ** (-0.5)).astype(jnp.bfloat16)
    mixed = lax.all_to_all(strip, "first", split_axis=0, concat_axis=2, tiled=True)
    scaled = norm_channels(mixed.astype(jnp.float32), mid_gain).astype(jnp.bfloat16)
    scaled = lax.optimization_barrier(scaled)
    gate = jax.nn.sigmoid(
        jnp.einsum("ijc,cd->ijd", ready, out_gate, preferred_element_type=jnp.float32)
    )
    return (
        jnp.einsum("ijd,dc->ijc", scaled, out_weight, preferred_element_type=jnp.float32) * gate
    ).astype(jnp.bfloat16)


def solution(mesh):
    in_specs = (P("first", "second", None), P(), P(), P(), P(), P(), P())
    out_specs = P("first", "second", None)
    planes, lines = mesh.shape["first"] // 2, mesh.shape["second"]
    if planes == lines == 4:
        body = functools.partial(triangle, planes, lines)
    else:
        body = shards
    return jax.shard_map(body, mesh=mesh, in_specs=in_specs, out_specs=out_specs, check_vma=False)
```

```python
import functools

import jax
import jax.numpy as jnp
from jax import lax
from jax.experimental import pallas as pl
from jax.experimental.pallas import tpu as pltpu
from jax.sharding import PartitionSpec as P

MESH = pl.DeviceIdType.MESH


def norm_channels(values, channel_gain):
    centred = values - jnp.mean(values, axis=-1, keepdims=True)
    return (
        centred
        * lax.rsqrt(jnp.mean(centred * centred, axis=-1, keepdims=True) + 1e-05)
        * channel_gain
    )


def dot(a, b):
    return jnp.dot(a, b, preferred_element_type=jnp.float32)


PIECE = 8
CHUNK = 2
DIRECT = 2


def other(index):
    return index + 1 - 2 * lax.rem(index, 2)


def centre(values, channel_gain):
    centred = values - jnp.mean(values, axis=-1, keepdims=True)
    scale = lax.rsqrt(jnp.mean(centred * centred, axis=-1, keepdims=True) + 1e-05)
    return (centred * channel_gain).astype(jnp.bfloat16), scale


def triangle_kernel(rows, cols, planes, lines, *refs):
    pieces, chunks = cols // PIECE, cols // CHUNK
    pl.run_scoped(
        functools.partial(triangle_steps, rows, cols, planes, lines, *refs),
        pltpu.SemaphoreType.DMA((6 + pieces,)),
        pltpu.SemaphoreType.DMA((lines, pieces)),
        pltpu.SemaphoreType.DMA((2, 2, pieces)),
        pltpu.SemaphoreType.DMA,
        pltpu.SemaphoreType.DMA,
        pltpu.SemaphoreType.DMA((2, chunks)),
        pltpu.SemaphoreType.DMA((2 * chunks + 4 * (chunks // 2),)),
        pltpu.SemaphoreType.REGULAR,
        pltpu.SemaphoreType.REGULAR,
        pltpu.SemaphoreType.REGULAR,
        pltpu.SemaphoreType.REGULAR,
    )


def triangle_steps(
    rows, cols, planes, lines,
    x_hbm, in_gain_hbm, left_w_hbm, right_w_hbm, mid_gain_hbm, out_w_hbm, gate_w_hbm,
    out_ref,
    x_ref, in_gain_ref, left_w_ref, right_w_ref, mid_gain_ref, out_w_ref, gate_w_ref,
    lsend, lrecv, rboth, left32, right32, psend, part32, inbox, gate,
    in_sem, lsend_sem, lrecv_sem, rsend_sem, rrecv_sem, psend_sem, inbox_sem, go_sem, across_sem, cross_sem, near_sem,
):
    first, second = lax.axis_index("first"), lax.axis_index("second")
    z, core = lax.div(first, 2), lax.rem(first, 2)
    pieces, chunks = cols // PIECE, cols // CHUNK
    per_piece, per_core = PIECE // CHUNK, chunks // 2
    lump, size = rows * PIECE, CHUNK * cols
    half = planes // 2
    upper, side, parity = lax.div(z, half), lax.div(second, half), lax.rem(second, 2)
    near_z = other(z)
    inner = lax.rem(z, 2) != upper
    outer = jnp.logical_not(inner)
    crossing = core == 1
    level = core == 0
    target_side = jnp.where(crossing, 1 - upper, upper)
    planes_of = [half * target_side + lax.rem(parity + u, 2) for u in range(2)]
    from_own = target_side == side
    is_own = [jnp.logical_and(level, planes_of[u] == z) for u in range(2)]
    is_near = [jnp.logical_and(level, planes_of[u] != z) for u in range(2)]
    x_second, y_second = other(second), lax.rem(second + half, lines)
    xy_second = other(y_second)
    cross_z = 2 * lax.rem(upper + 1, 2) + lax.rem(upper + 1 + 1, 2)

    def device(z_at, core_at, second_at):
        return {"first": 2 * z_at + core_at, "second": second_at}

    scope = jax.named_scope
    barrier = pltpu.get_barrier_semaphore()

    def greet(z_at, core_at, second_at):
        pl.semaphore_signal(
            barrier, inc=1, device_id=device(z_at, core_at, second_at), device_id_type=MESH
        )

    target = lax.rem(side + upper, 2)
    early = jnp.logical_and(crossing, jnp.logical_and(inner, upper == 0))
    even = lax.rem(z, 2) == 0
    far_target = jnp.logical_and(jnp.logical_and(crossing, upper == 0), lax.rem(z, 2) != parity)
    last_column = second == lines - 1
    slow_column = second == half

    with scope("sig"):
        greet(z, 1 - core, second)

        @pl.when(far_target)
        def _():
            greet(planes - 1, 1, second)

        for c in range(2):

            @pl.when(from_own)
            def _():
                greet(z, c, x_second)

            @pl.when(jnp.logical_not(from_own))
            def _():
                greet(z, c, y_second)

        @pl.when(jnp.logical_and(crossing, jnp.logical_not(last_column)))
        def _():
            greet(z, 1, x_second)

        @pl.when(jnp.logical_and(second == 0, jnp.logical_not(from_own)))
        def _():
            for c in range(2):
                greet(z, c, xy_second)

        @pl.when(even)
        def _():
            greet(near_z, 0, second)

            @pl.when(level)
            def _():
                for c in range(2):
                    greet(near_z, c, second)

            @pl.when(crossing)
            def _():
                greet(near_z, 1, second)

        @pl.when(upper == 0)
        def _():
            greet(cross_z, 1, second)

        @pl.when(early)
        def _():
            for dz in range(half):
                for c in range(2):
                    greet(half + dz, c, second)

    loads = [
        pltpu.make_async_copy(src, dst, in_sem.at[n])
        for n, (src, dst) in enumerate((
            (in_gain_hbm, in_gain_ref), (left_w_hbm, left_w_ref),
            *((x_hbm.at[:, pl.ds(c * PIECE, PIECE), :], x_ref.at[c]) for c in range(pieces)),
            (right_w_hbm, right_w_ref),
            (gate_w_hbm, gate_w_ref), (mid_gain_hbm, mid_gain_ref), (out_w_hbm, out_w_ref),
        ))
    ]
    for load in loads:
        load.start()
    def meet():
        signals = (
            3
            + jnp.where(even, 0, 1 + jnp.where(level, 2, 1))
            + jnp.where(jnp.logical_and(crossing, z == half), 2 * half, 0)
            + jnp.where(jnp.logical_and(crossing, z == planes - 1), 1, 0)
            + jnp.where(last_column, 1, 0)
            + jnp.where(jnp.logical_and(crossing, second != half), 1, 0)
            + upper
        )
        pl.semaphore_wait(barrier, signals.astype(jnp.int32))

        def answer(semaphore, z_at, core_at, second_at):
            pl.semaphore_signal(
                semaphore, inc=1, device_id=device(z_at, core_at, second_at), device_id_type=MESH
            )

        @pl.when(jnp.logical_and(crossing, second != half))
        def _():
            answer(across_sem, z, 1, x_second)

        @pl.when(jnp.logical_not(even))
        def _():
            answer(near_sem, near_z, 0, second)

        @pl.when(early)
        def _():
            answer(near_sem, near_z, 1, second)

        @pl.when(upper == 1)
        def _():
            answer(cross_sem, cross_z, 1, second)

    with scope("bar"):
        pl.when(last_column)(meet)

    def left_copy(t, c):
        return pltpu.make_async_remote_copy(
            src_ref=lsend.at[c],
            dst_ref=lrecv.at[t % 2, core, c],
            send_sem=lsend_sem.at[t, c],
            recv_sem=lrecv_sem.at[t % 2, core, c],
            device_id=device(z, target, (second, x_second, y_second, xy_second)[t]),
            device_id_type=MESH,
        )

    with scope("load"):
        loads[0].wait()
        loads[1].wait()

    def send_left(c):
        for t in (2, 1):
            left_copy(t, c).start()

        @pl.when(target != core)
        def _():
            left_copy(0, c).start()

    ready, scales = [], []
    for c in range(pieces):
        with scope(f"left{c}"):
            loads[2 + c].wait()
            x = x_ref[c].astype(jnp.float32).reshape(lump, x_ref.shape[-1])
            for list_of, value in zip((ready, scales), centre(x, in_gain_ref[...])):
                list_of.append(value)
            lsend[c] = (dot(ready[c], left_w_ref[...]) * scales[c]).astype(jnp.bfloat16)
        if c == 0:
            with scope("bar0"):
                pl.when(side == 0)(meet)

        @pl.when(jnp.logical_not(slow_column))
        def _():
            send_left(c)

    with scope("right"):
        loads[pieces + 2].wait()
        ready, scales = (jnp.concatenate(list_of, axis=0) for list_of in (ready, scales))
        right = (dot(ready, right_w_ref[...]) * scales).astype(jnp.bfloat16)
        rboth[core] = right
    with scope("bar2"):

        @pl.when(slow_column)
        def _():
            meet()
            for c in range(pieces):
                send_left(c)

    right_copy = pltpu.make_async_remote_copy(
        src_ref=rboth.at[core],
        dst_ref=rboth.at[core],
        send_sem=rsend_sem,
        recv_sem=rrecv_sem,
        device_id=device(z, 1 - core, second),
        device_id_type=MESH,
    )
    right_copy.start()
    with scope("across"):
        @pl.when(jnp.logical_not(last_column))
        def _():
            pl.semaphore_wait(across_sem, 1)

            @pl.when(crossing)
            def _():
                pl.semaphore_signal(
                    across_sem, inc=1, device_id=device(z, 0, second), device_id_type=MESH
                )

        for c in range(pieces):
            left_copy(3, c).start()
    with scope("gate"):
        loads[pieces + 3].wait()
        gates = jax.nn.sigmoid(dot(ready, gate_w_ref[...]) * scales)
        for c in range(pieces):
            for k in range(rows):
                at = c * lump + k * PIECE
                gate[k * cols + c * PIECE : k * cols + (c + 1) * PIECE, :] = gates[at : at + PIECE, :]
        loads[pieces + 4].wait()
        loads[pieces + 5].wait()

    with scope("rwait"):
        right_copy.wait_recv()
    with scope("r32"):
        for q in range(2):
            right32[q] = rboth[q].astype(jnp.float32)

    def send(j, n, slot, to):
        return pltpu.make_async_remote_copy(
            src_ref=psend.at[j, n],
            dst_ref=inbox.at[slot],
            send_sem=psend_sem.at[j, n],
            recv_sem=inbox_sem.at[slot],
            device_id=to,
            device_id_type=MESH,
        )

    near_at, cross_at, own_at, far_at = (2 * chunks + n * per_core for n in range(4))
    descending = jnp.logical_and(crossing, upper == 1)

    def waits(j, n):
        return j == 0 and n >= per_core

    def skips(j, n):
        return j == 1 and n >= chunks - DIRECT

    near_early = jnp.logical_and(upper == side, parity != lax.rem(z, 2))
    held_back = outer

    def relay_copy(j, n):
        return send(j, n, j * chunks + n, device(near_z, 1, second))

    def far_copy(j, n):
        return send(j, n, far_at + n % per_core, device(planes_of[j], 1, second))

    def near_copy(j, n):
        return send(j, n, near_at + n % per_core, device(near_z, n // per_core, second))

    def cross_copy(j, n):
        return send(j, n, cross_at + n % per_core, device(planes_of[j], n // per_core, second))

    def own_copy(j, n):
        return send(j, n, own_at + n % per_core, device(z, 1, second))

    def block(j, c):
        with scope(f"wl{j}{c}"):
            for q in range(2):
                mine = jnp.logical_and(from_own, core == q) if j == 0 else None

                def arrived():
                    pltpu.make_async_remote_copy(
                        src_ref=lsend.at[c],
                        dst_ref=lrecv.at[j, q, c],
                        send_sem=lsend_sem.at[0, c],
                        recv_sem=lrecv_sem.at[j, q, c],
                        device_id=device(z, 1 - core, second),
                        device_id_type=MESH,
                    ).wait_recv()
                    left32[c, q] = lrecv[j, q, c].astype(jnp.float32)

                if j:
                    arrived()
                else:
                    pl.when(jnp.logical_not(mine))(arrived)

                    @pl.when(mine)
                    def _():
                        left32[c, q] = lsend[c].astype(jnp.float32)

        with scope(f"block{j}{c}"):
            for part in range(per_piece):
                n = c * per_piece + part
                sums = tuple(jnp.zeros((cols, x_ref.shape[-1]), jnp.float32) for _ in range(CHUNK))
                for q in range(2):

                    def body(k, sums):
                        at = pl.multiple_of(k * PIECE, PIECE)
                        r = jnp.concatenate(
                            [right32[q, pl.ds(p * lump + at, PIECE), :] for p in range(pieces)], axis=0
                        )
                        return tuple(
                            total + left32[c, q, pl.ds(at + part * CHUNK + i, 1), :] * r
                            for i, total in enumerate(sums)
                        )

                    sums = lax.fori_loop(0, rows, body, sums, unroll=True)
                total = jnp.concatenate(sums, axis=0)

                @pl.when(jnp.logical_and(crossing, inner))
                def _():
                    part32[j, n] = total

                psend[j, n] = total.astype(jnp.bfloat16)

                sends = jnp.logical_and(crossing, outer)
                if skips(j, n):
                    sends = jnp.logical_and(sends, upper == 0)
                if waits(j, n):
                    sends = jnp.logical_and(sends, parity == 0)

                @pl.when(sends)
                def _():
                    relay_copy(j, n).start()

                if skips(j, n):

                    @pl.when(jnp.logical_and(descending, outer))
                    def _():
                        far_copy(j, n).start()

                    @pl.when(jnp.logical_and(descending, inner))
                    def _():
                        cross_copy(j, n).start()

                @pl.when(is_own[j])
                def _():
                    if n < per_core:
                        inbox[own_at + n] = psend[j, n]
                    else:
                        own_copy(j, n).start()

                @pl.when(jnp.logical_and(is_near[j], jnp.logical_not(held_back)))
                def _():
                    near_copy(j, n).start()

    with scope("nearbar"):

        @pl.when(jnp.logical_and(even, level))
        def _():
            pl.semaphore_wait(near_sem, 2)

        @pl.when(jnp.logical_and(z == 0, crossing))
        def _():
            pl.semaphore_wait(near_sem, 1)

    for j in range(2):
        for c in range(pieces):
            block(j, c)

    by_plane = [(j, n) for j in range(2) for n in range(chunks)]
    by_need = sorted(by_plane, key=lambda at: waits(*at))
    with scope("late"):

        @pl.when(jnp.logical_and(jnp.logical_and(crossing, outer), parity == 1))
        def _():
            for j, n in by_plane:
                if waits(j, n):
                    relay_copy(j, n).start()

    with scope("relay"):

        @pl.when(early)
        def _():
            pl.semaphore_wait(cross_sem, 2 * half)

        @pl.when(jnp.logical_and(crossing, inner))
        def _():
            def relay(j, n):
                relay_copy(j, n).wait_recv()
                total = part32[j, n] + inbox[j * chunks + n].astype(jnp.float32)
                psend[j, n] = total.astype(jnp.bfloat16)
                cross_copy(j, n).start()

            def relay_all(order):
                for j, n in order:
                    if skips(j, n):
                        pl.when(upper == 0)(functools.partial(relay, j, n))
                    else:
                        relay(j, n)

            pl.when(parity == 0)(lambda: relay_all(by_plane))
            pl.when(parity == 1)(lambda: relay_all(by_need))

    cuts = (by_plane, 2 * chunks - chunks // 4), (by_need, 2 * chunks - per_core)

    def wait_sent(order):
        for j, n in order:
            near_copy(j, n).wait_send()

    with scope("held"):

        @pl.when(held_back)
        def _():
            @pl.when(crossing)
            def _():
                for odd, (order, cut) in enumerate(cuts):
                    pl.when(parity == odd)(functools.partial(wait_sent, order[:cut]))
                pl.semaphore_signal(go_sem, inc=1, device_id=device(z, 0, second), device_id_type=MESH)

            @pl.when(level)
            def _():
                pl.semaphore_wait(go_sem, 1)
                for j in range(2):

                    @pl.when(is_near[j])
                    def _():
                        for n in range(chunks):
                            near_copy(j, n).start()

    count = rows * 2 * planes
    for c in range(per_core):
        with scope(f"own{c}"):

            @pl.when(crossing)
            def _():
                own_copy(0, c).wait_recv()

        with scope(f"near{c}"):
            near_copy(0, c).wait_recv()
    with scope("sum"):
        for c in range(per_core):
            part32[0, c] = inbox[own_at + c].astype(jnp.float32) + inbox[near_at + c].astype(jnp.float32)
    with scope("drain"):
        for t in (1, 2, 3):
            for c in range(pieces):
                left_copy(t, c).wait_send()

        @pl.when(target != core)
        def _():
            for c in range(pieces):
                left_copy(0, c).wait_send()

        right_copy.wait_send()

        @pl.when(crossing)
        def _():
            for odd, (order, cut) in enumerate(cuts):

                @pl.when(parity == odd)
                def _():
                    wait_sent(order[cut:])
                    pl.when(jnp.logical_not(held_back))(functools.partial(wait_sent, order[:cut]))

    def drain_level():
        for j, n in by_plane:
            if n < per_core:

                @pl.when(is_near[j])
                def _():
                    near_copy(j, n).wait_send()

            else:
                near_copy(j, n).wait_send()

    pl.when(jnp.logical_and(level, jnp.logical_not(held_back)))(drain_level)
    with scope("cross"):
        for c in range(per_core):
            cross_copy(0, c).wait_recv()
    with scope("far"):

        @pl.when(far_target)
        def _():
            for c in range(per_core - DIRECT, per_core):
                part32[0, c] = part32[0, c] + inbox[cross_at + c].astype(jnp.float32)
                send(0, c, far_at + c, device(near_z, 0, second)).wait_recv()

    last_at = [
        (jnp.where(far_target, far_at, cross_at) if c >= per_core - DIRECT else cross_at) + c
        for c in range(per_core)
    ]
    with scope("final"):
        total = jnp.concatenate(
            [part32[0, c] + inbox[last_at[c]].astype(jnp.float32) for c in range(per_core)], axis=0
        )
        mixed = (total * count ** (-0.5)).astype(jnp.bfloat16)
        scaled, scale = centre(mixed.astype(jnp.float32), mid_gain_ref[...])
        out_ref[...] = (dot(scaled, out_w_ref[...]) * (gate[...] * scale)).astype(jnp.bfloat16)

    pl.when(jnp.logical_and(level, held_back))(drain_level)


def triangle(planes, lines, pair_rows, in_gain, left_weight, right_weight, mid_gain, out_weight, out_gate):
    rows, cols, width = pair_rows.shape
    mix = left_weight.shape[1]
    pairs, pieces, chunks, size = rows * cols, cols // PIECE, cols // CHUNK, CHUNK * cols
    lump = rows * PIECE
    slots = 2 * chunks + 4 * (chunks // 2)
    anywhere = pl.BlockSpec(memory_space=pl.ANY)
    bf16, f32 = jnp.bfloat16, jnp.float32
    out = pl.pallas_call(
        functools.partial(triangle_kernel, rows, cols, planes, lines),
        out_shape=pltpu.VMEM((pairs, width), bf16),
        in_specs=[anywhere] * 7,
        out_specs=pl.BlockSpec(memory_space=pltpu.VMEM),
        scratch_shapes=[
            pltpu.VMEM((pieces, rows, PIECE, width), bf16),
            pltpu.VMEM((1, width), f32),
            pltpu.VMEM((width, mix), bf16),
            pltpu.VMEM((width, mix), bf16),
            pltpu.VMEM((1, mix), f32),
            pltpu.VMEM((mix, width), bf16),
            pltpu.VMEM((width, width), bf16),
            pltpu.VMEM((pieces, lump, mix), bf16),
            pltpu.VMEM((2, 2, pieces, lump, mix), bf16),
            pltpu.VMEM((2, pairs, mix), bf16),
            pltpu.VMEM((pieces, 2, lump, mix), f32),
            pltpu.VMEM((2, pairs, mix), f32),
            pltpu.VMEM((2, chunks, size, mix), bf16),
            pltpu.VMEM((2, chunks, size, mix), f32),
            pltpu.VMEM((slots, size, mix), bf16),
            pltpu.VMEM((pairs, width), f32),
        ],
        compiler_params=pltpu.CompilerParams(collective_id=0, has_side_effects=True),
    )(
        pair_rows, in_gain.reshape(1, width), left_weight, right_weight,
        mid_gain.reshape(1, mix), out_weight, out_gate,
    )
    return out.reshape(rows, cols, width)


def shards(pair_rows, in_gain, left_weight, right_weight, mid_gain, out_weight, out_gate):
    ready = norm_channels(pair_rows.astype(jnp.float32), in_gain).astype(jnp.bfloat16)
    ready = lax.optimization_barrier(ready)
    left = jnp.einsum("ijc,cd->ijd", ready, left_weight, preferred_element_type=jnp.float32)
    right = jnp.einsum("ijc,cd->ijd", ready, right_weight, preferred_element_type=jnp.float32)
    left, right = left.astype(jnp.bfloat16), right.astype(jnp.bfloat16)
    count = pair_rows.shape[0] * lax.axis_size("first")
    left_lines, right_lines = (
        lax.all_to_all(left, "first", split_axis=2, concat_axis=0, tiled=True),
        lax.all_to_all(right, "first", split_axis=2, concat_axis=0, tiled=True),
    )
    strip = jnp.einsum(
        "kid,kjd->ijd",
        lax.all_gather(left_lines, "second", axis=1, tiled=True),
        right_lines,
        preferred_element_type=jnp.float32,
    )
    strip = (strip * count ** (-0.5)).astype(jnp.bfloat16)
    mixed = lax.all_to_all(strip, "first", split_axis=0, concat_axis=2, tiled=True)
    scaled = norm_channels(mixed.astype(jnp.float32), mid_gain).astype(jnp.bfloat16)
    scaled = lax.optimization_barrier(scaled)
    gate = jax.nn.sigmoid(
        jnp.einsum("ijc,cd->ijd", ready, out_gate, preferred_element_type=jnp.float32)
    )
    return (
        jnp.einsum("ijd,dc->ijc", scaled, out_weight, preferred_element_type=jnp.float32) * gate
    ).astype(jnp.bfloat16)


def solution(mesh):
    in_specs = (P("first", "second", None), P(), P(), P(), P(), P(), P())
    out_specs = P("first", "second", None)
    planes, lines = mesh.shape["first"] // 2, mesh.shape["second"]
    if planes == lines == 4:
        body = functools.partial(triangle, planes, lines)
    else:
        body = shards
    return jax.shard_map(body, mesh=mesh, in_specs=in_specs, out_specs=out_specs, check_vma=False)
```

```python
import functools

import jax
import jax.numpy as jnp
from jax import lax
from jax.experimental import pallas as pl
from jax.experimental.pallas import tpu as pltpu
from jax.sharding import PartitionSpec as P

MESH = pl.DeviceIdType.MESH


def norm_channels(values, channel_gain):
    centred = values - jnp.mean(values, axis=-1, keepdims=True)
    return (
        centred
        * lax.rsqrt(jnp.mean(centred * centred, axis=-1, keepdims=True) + 1e-05)
        * channel_gain
    )


def dot(a, b):
    return jnp.dot(a, b, preferred_element_type=jnp.float32)


PIECE = 8
CHUNK = 2
DIRECT = 2


def other(index):
    return index + 1 - 2 * lax.rem(index, 2)


def centre(values, channel_gain):
    centred = values - jnp.mean(values, axis=-1, keepdims=True)
    scale = lax.rsqrt(jnp.mean(centred * centred, axis=-1, keepdims=True) + 1e-05)
    return (centred * channel_gain).astype(jnp.bfloat16), scale


def triangle_kernel(rows, cols, planes, lines, *refs):
    pieces, chunks = cols // PIECE, cols // CHUNK
    pl.run_scoped(
        functools.partial(triangle_steps, rows, cols, planes, lines, *refs),
        pltpu.SemaphoreType.DMA((6 + pieces,)),
        pltpu.SemaphoreType.DMA((lines, pieces)),
        pltpu.SemaphoreType.DMA((2, 2, pieces)),
        pltpu.SemaphoreType.DMA,
        pltpu.SemaphoreType.DMA,
        pltpu.SemaphoreType.DMA((2, chunks)),
        pltpu.SemaphoreType.DMA((2 * chunks + 4 * (chunks // 2),)),
        pltpu.SemaphoreType.REGULAR,
        pltpu.SemaphoreType.REGULAR,
        pltpu.SemaphoreType.REGULAR,
        pltpu.SemaphoreType.REGULAR,
    )


def triangle_steps(
    rows, cols, planes, lines,
    x_hbm, in_gain_hbm, left_w_hbm, right_w_hbm, mid_gain_hbm, out_w_hbm, gate_w_hbm,
    out_ref,
    x_ref, in_gain_ref, left_w_ref, right_w_ref, mid_gain_ref, out_w_ref, gate_w_ref,
    lsend, lrecv, rboth, left32, right32, psend, part32, inbox, gate,
    in_sem, lsend_sem, lrecv_sem, rsend_sem, rrecv_sem, psend_sem, inbox_sem, go_sem, across_sem, cross_sem, near_sem,
):
    first, second = lax.axis_index("first"), lax.axis_index("second")
    z, core = lax.div(first, 2), lax.rem(first, 2)
    pieces, chunks = cols // PIECE, cols // CHUNK
    per_piece, per_core = PIECE // CHUNK, chunks // 2
    lump, size = rows * PIECE, CHUNK * cols
    half = planes // 2
    upper, side, parity = lax.div(z, half), lax.div(second, half), lax.rem(second, 2)
    near_z = other(z)
    inner = lax.rem(z, 2) != upper
    outer = jnp.logical_not(inner)
    crossing = core == 1
    level = core == 0
    target_side = jnp.where(crossing, 1 - upper, upper)
    planes_of = [half * target_side + lax.rem(parity + u, 2) for u in range(2)]
    from_own = target_side == side
    is_own = [jnp.logical_and(level, planes_of[u] == z) for u in range(2)]
    is_near = [jnp.logical_and(level, planes_of[u] != z) for u in range(2)]
    x_second, y_second = other(second), lax.rem(second + half, lines)
    xy_second = other(y_second)
    cross_z = 2 * lax.rem(upper + 1, 2) + lax.rem(upper + 1 + 1, 2)

    def device(z_at, core_at, second_at):
        return {"first": 2 * z_at + core_at, "second": second_at}

    scope = jax.named_scope
    barrier = pltpu.get_barrier_semaphore()

    def greet(z_at, core_at, second_at):
        pl.semaphore_signal(
            barrier, inc=1, device_id=device(z_at, core_at, second_at), device_id_type=MESH
        )

    target = lax.rem(side + upper, 2)
    early = jnp.logical_and(crossing, jnp.logical_and(inner, upper == 0))
    even = lax.rem(z, 2) == 0
    far_target = jnp.logical_and(jnp.logical_and(crossing, upper == 0), lax.rem(z, 2) != parity)
    last_column = second == lines - 1
    slow_column = second == half

    with scope("sig"):
        greet(z, 1 - core, second)

        @pl.when(far_target)
        def _():
            greet(planes - 1, 1, second)

        for c in range(2):

            @pl.when(from_own)
            def _():
                greet(z, c, x_second)

            @pl.when(jnp.logical_not(from_own))
            def _():
                greet(z, c, y_second)

        @pl.when(jnp.logical_and(crossing, jnp.logical_not(last_column)))
        def _():
            greet(z, 1, x_second)

        @pl.when(jnp.logical_and(second == 0, jnp.logical_not(from_own)))
        def _():
            for c in range(2):
                greet(z, c, xy_second)

        @pl.when(even)
        def _():
            greet(near_z, 0, second)

            @pl.when(level)
            def _():
                for c in range(2):
                    greet(near_z, c, second)

            @pl.when(crossing)
            def _():
                greet(near_z, 1, second)

        @pl.when(upper == 0)
        def _():
            greet(cross_z, 1, second)

        @pl.when(early)
        def _():
            for dz in range(half):
                for c in range(2):
                    greet(half + dz, c, second)

    loads = [
        pltpu.make_async_copy(src, dst, in_sem.at[n])
        for n, (src, dst) in enumerate((
            (in_gain_hbm, in_gain_ref), (left_w_hbm, left_w_ref),
            *((x_hbm.at[:, pl.ds(c * PIECE, PIECE), :], x_ref.at[c]) for c in range(pieces)),
            (right_w_hbm, right_w_ref),
            (gate_w_hbm, gate_w_ref), (mid_gain_hbm, mid_gain_ref), (out_w_hbm, out_w_ref),
        ))
    ]
    for load in loads:
        load.start()
    def meet():
        signals = (
            3
            + jnp.where(even, 0, 1 + jnp.where(level, 2, 1))
            + jnp.where(jnp.logical_and(crossing, z == half), 2 * half, 0)
            + jnp.where(jnp.logical_and(crossing, z == planes - 1), 1, 0)
            + jnp.where(last_column, 1, 0)
            + jnp.where(jnp.logical_and(crossing, second != half), 1, 0)
            + upper
        )
        pl.semaphore_wait(barrier, signals.astype(jnp.int32))

        def answer(semaphore, z_at, core_at, second_at):
            pl.semaphore_signal(
                semaphore, inc=1, device_id=device(z_at, core_at, second_at), device_id_type=MESH
            )

        @pl.when(jnp.logical_and(crossing, second != half))
        def _():
            answer(across_sem, z, 1, x_second)

        @pl.when(jnp.logical_not(even))
        def _():
            answer(near_sem, near_z, 0, second)

        @pl.when(early)
        def _():
            answer(near_sem, near_z, 1, second)

        @pl.when(upper == 1)
        def _():
            answer(cross_sem, cross_z, 1, second)

    with scope("bar"):
        pl.when(last_column)(meet)

    def left_copy(t, c):
        return pltpu.make_async_remote_copy(
            src_ref=lsend.at[c],
            dst_ref=lrecv.at[t % 2, core, c],
            send_sem=lsend_sem.at[t, c],
            recv_sem=lrecv_sem.at[t % 2, core, c],
            device_id=device(z, target, (second, x_second, y_second, xy_second)[t]),
            device_id_type=MESH,
        )

    with scope("load"):
        loads[0].wait()
        loads[1].wait()

    def send_left(c):
        for t in (2, 1):
            left_copy(t, c).start()

        @pl.when(target != core)
        def _():
            left_copy(0, c).start()

    ready, scales = [], []
    for c in range(pieces):
        with scope(f"left{c}"):
            loads[2 + c].wait()
            x = x_ref[c].astype(jnp.float32).reshape(lump, x_ref.shape[-1])
            for list_of, value in zip((ready, scales), centre(x, in_gain_ref[...])):
                list_of.append(value)
            lsend[c] = (dot(ready[c], left_w_ref[...]) * scales[c]).astype(jnp.bfloat16)
        if c == 0:
            with scope("bar0"):
                pl.when(side == 0)(meet)

        @pl.when(jnp.logical_not(slow_column))
        def _():
            send_left(c)

    with scope("right"):
        loads[pieces + 2].wait()
        ready, scales = (jnp.concatenate(list_of, axis=0) for list_of in (ready, scales))
        right = (dot(ready, right_w_ref[...]) * scales).astype(jnp.bfloat16)
        rboth[core] = right
    with scope("bar2"):

        @pl.when(slow_column)
        def _():
            meet()
            for c in range(pieces):
                send_left(c)

    right_copy = pltpu.make_async_remote_copy(
        src_ref=rboth.at[core],
        dst_ref=rboth.at[core],
        send_sem=rsend_sem,
        recv_sem=rrecv_sem,
        device_id=device(z, 1 - core, second),
        device_id_type=MESH,
    )
    right_copy.start()
    with scope("across"):
        @pl.when(jnp.logical_not(last_column))
        def _():
            pl.semaphore_wait(across_sem, 1)

            @pl.when(crossing)
            def _():
                pl.semaphore_signal(
                    across_sem, inc=1, device_id=device(z, 0, second), device_id_type=MESH
                )

        for c in range(pieces):
            left_copy(3, c).start()
    with scope("gate"):
        loads[pieces + 3].wait()
        gates = jax.nn.sigmoid(dot(ready, gate_w_ref[...]) * scales)
        for c in range(pieces):
            for k in range(rows):
                at = c * lump + k * PIECE
                gate[k * cols + c * PIECE : k * cols + (c + 1) * PIECE, :] = gates[at : at + PIECE, :]
        loads[pieces + 4].wait()
        loads[pieces + 5].wait()

    with scope("rwait"):
        right_copy.wait_recv()
    with scope("r32"):
        for q in range(2):
            right32[q] = rboth[q].astype(jnp.float32)

    def send(j, n, slot, to):
        return pltpu.make_async_remote_copy(
            src_ref=psend.at[j, n],
            dst_ref=inbox.at[slot],
            send_sem=psend_sem.at[j, n],
            recv_sem=inbox_sem.at[slot],
            device_id=to,
            device_id_type=MESH,
        )

    near_at, cross_at, own_at, far_at = (2 * chunks + n * per_core for n in range(4))
    descending = jnp.logical_and(crossing, upper == 1)

    def waits(j, n):
        return j == 0 and n >= per_core

    def skips(j, n):
        return j == 1 and n >= chunks - DIRECT

    near_early = jnp.logical_and(upper == side, parity != lax.rem(z, 2))
    held_back = outer

    def relay_copy(j, n):
        return send(j, n, j * chunks + n, device(near_z, 1, second))

    def far_copy(j, n):
        return send(j, n, far_at + n % per_core, device(planes_of[j], 1, second))

    def near_copy(j, n):
        return send(j, n, near_at + n % per_core, device(near_z, n // per_core, second))

    def cross_copy(j, n):
        return send(j, n, cross_at + n % per_core, device(planes_of[j], n // per_core, second))

    def own_copy(j, n):
        return send(j, n, own_at + n % per_core, device(z, 1, second))

    def block(j, c):
        with scope(f"wl{j}{c}"):
            for q in range(2):
                mine = jnp.logical_and(from_own, core == q) if j == 0 else None

                def arrived():
                    pltpu.make_async_remote_copy(
                        src_ref=lsend.at[c],
                        dst_ref=lrecv.at[j, q, c],
                        send_sem=lsend_sem.at[0, c],
                        recv_sem=lrecv_sem.at[j, q, c],
                        device_id=device(z, 1 - core, second),
                        device_id_type=MESH,
                    ).wait_recv()
                    left32[c, q] = lrecv[j, q, c].astype(jnp.float32)

                if j:
                    arrived()
                else:
                    pl.when(jnp.logical_not(mine))(arrived)

                    @pl.when(mine)
                    def _():
                        left32[c, q] = lsend[c].astype(jnp.float32)

        with scope(f"block{j}{c}"):
            for part in range(per_piece):
                n = c * per_piece + part
                sums = tuple(jnp.zeros((cols, x_ref.shape[-1]), jnp.float32) for _ in range(CHUNK))
                for q in range(2):

                    def body(k, sums):
                        at = pl.multiple_of(k * PIECE, PIECE)
                        r = jnp.concatenate(
                            [right32[q, pl.ds(p * lump + at, PIECE), :] for p in range(pieces)], axis=0
                        )
                        return tuple(
                            total + left32[c, q, pl.ds(at + part * CHUNK + i, 1), :] * r
                            for i, total in enumerate(sums)
                        )

                    sums = lax.fori_loop(0, rows, body, sums, unroll=True)
                total = jnp.concatenate(sums, axis=0)

                @pl.when(jnp.logical_and(crossing, inner))
                def _():
                    part32[j, n] = total

                psend[j, n] = total.astype(jnp.bfloat16)

                sends = jnp.logical_and(crossing, outer)
                if skips(j, n):
                    sends = jnp.logical_and(sends, upper == 0)
                if waits(j, n):
                    sends = jnp.logical_and(sends, parity == 0)

                @pl.when(sends)
                def _():
                    relay_copy(j, n).start()

                if skips(j, n):

                    @pl.when(jnp.logical_and(descending, outer))
                    def _():
                        far_copy(j, n).start()

                    @pl.when(jnp.logical_and(descending, inner))
                    def _():
                        cross_copy(j, n).start()

                @pl.when(is_own[j])
                def _():
                    if n < per_core:
                        inbox[own_at + n] = psend[j, n]
                    else:
                        own_copy(j, n).start()

                @pl.when(jnp.logical_and(is_near[j], jnp.logical_not(held_back)))
                def _():
                    near_copy(j, n).start()

    with scope("nearbar"):

        @pl.when(jnp.logical_and(even, level))
        def _():
            pl.semaphore_wait(near_sem, 2)

        @pl.when(jnp.logical_and(z == 0, crossing))
        def _():
            pl.semaphore_wait(near_sem, 1)

    for j in range(2):
        for c in range(pieces):
            block(j, c)

    by_plane = [(j, n) for j in range(2) for n in range(chunks)]
    by_need = sorted(by_plane, key=lambda at: waits(*at))
    with scope("late"):

        @pl.when(jnp.logical_and(jnp.logical_and(crossing, outer), parity == 1))
        def _():
            for j, n in by_plane:
                if waits(j, n):
                    relay_copy(j, n).start()

    with scope("relay"):

        @pl.when(early)
        def _():
            pl.semaphore_wait(cross_sem, 2 * half)

        @pl.when(jnp.logical_and(crossing, inner))
        def _():
            def relay(j, n):
                relay_copy(j, n).wait_recv()
                total = part32[j, n] + inbox[j * chunks + n].astype(jnp.float32)
                psend[j, n] = total.astype(jnp.bfloat16)
                cross_copy(j, n).start()

            def relay_all(order):
                for j, n in order:
                    if skips(j, n):
                        pl.when(upper == 0)(functools.partial(relay, j, n))
                    else:
                        relay(j, n)

            pl.when(parity == 0)(lambda: relay_all(by_plane))
            pl.when(parity == 1)(lambda: relay_all(by_need))

    cuts = (by_plane, 2 * chunks - chunks // 4), (by_need, 2 * chunks - per_core)

    def wait_sent(order):
        for j, n in order:
            near_copy(j, n).wait_send()

    with scope("held"):

        @pl.when(held_back)
        def _():
            @pl.when(crossing)
            def _():
                for odd, (order, cut) in enumerate(cuts):
                    pl.when(parity == odd)(functools.partial(wait_sent, order[:cut]))
                pl.semaphore_signal(go_sem, inc=1, device_id=device(z, 0, second), device_id_type=MESH)

            @pl.when(level)
            def _():
                pl.semaphore_wait(go_sem, 1)
                for j in range(2):

                    @pl.when(is_near[j])
                    def _():
                        for n in range(chunks):
                            near_copy(j, n).start()

    count = rows * 2 * planes
    with scope("drain"):
        for t in (1, 2, 3):
            for c in range(pieces):
                left_copy(t, c).wait_send()

        @pl.when(target != core)
        def _():
            for c in range(pieces):
                left_copy(0, c).wait_send()

        right_copy.wait_send()

        @pl.when(crossing)
        def _():
            for odd, (order, cut) in enumerate(cuts):

                @pl.when(parity == odd)
                def _():
                    wait_sent(order[cut:])
                    pl.when(jnp.logical_not(held_back))(functools.partial(wait_sent, order[:cut]))

    def drain_level():
        for j, n in by_plane:
            if n < per_core:

                @pl.when(is_near[j])
                def _():
                    near_copy(j, n).wait_send()

            else:
                near_copy(j, n).wait_send()

    pl.when(jnp.logical_and(level, jnp.logical_not(held_back)))(drain_level)
    for c in range(per_core):
        with scope(f"own{c}"):

            @pl.when(crossing)
            def _():
                own_copy(0, c).wait_recv()

        with scope(f"near{c}"):
            near_copy(0, c).wait_recv()
    with scope("sum"):
        for c in range(per_core):
            part32[0, c] = inbox[own_at + c].astype(jnp.float32) + inbox[near_at + c].astype(jnp.float32)
    with scope("cross"):
        for c in range(per_core):
            cross_copy(0, c).wait_recv()
    with scope("far"):

        @pl.when(far_target)
        def _():
            for c in range(per_core - DIRECT, per_core):
                part32[0, c] = part32[0, c] + inbox[cross_at + c].astype(jnp.float32)
                send(0, c, far_at + c, device(near_z, 0, second)).wait_recv()

    last_at = [
        (jnp.where(far_target, far_at, cross_at) if c >= per_core - DIRECT else cross_at) + c
        for c in range(per_core)
    ]
    with scope("final"):
        total = jnp.concatenate(
            [part32[0, c] + inbox[last_at[c]].astype(jnp.float32) for c in range(per_core)], axis=0
        )
        mixed = (total * count ** (-0.5)).astype(jnp.bfloat16)
        scaled, scale = centre(mixed.astype(jnp.float32), mid_gain_ref[...])
        out_ref[...] = (dot(scaled, out_w_ref[...]) * (gate[...] * scale)).astype(jnp.bfloat16)

    pl.when(jnp.logical_and(level, held_back))(drain_level)


def triangle(planes, lines, pair_rows, in_gain, left_weight, right_weight, mid_gain, out_weight, out_gate):
    rows, cols, width = pair_rows.shape
    mix = left_weight.shape[1]
    pairs, pieces, chunks, size = rows * cols, cols // PIECE, cols // CHUNK, CHUNK * cols
    lump = rows * PIECE
    slots = 2 * chunks + 4 * (chunks // 2)
    anywhere = pl.BlockSpec(memory_space=pl.ANY)
    bf16, f32 = jnp.bfloat16, jnp.float32
    out = pl.pallas_call(
        functools.partial(triangle_kernel, rows, cols, planes, lines),
        out_shape=pltpu.VMEM((pairs, width), bf16),
        in_specs=[anywhere] * 7,
        out_specs=pl.BlockSpec(memory_space=pltpu.VMEM),
        scratch_shapes=[
            pltpu.VMEM((pieces, rows, PIECE, width), bf16),
            pltpu.VMEM((1, width), f32),
            pltpu.VMEM((width, mix), bf16),
            pltpu.VMEM((width, mix), bf16),
            pltpu.VMEM((1, mix), f32),
            pltpu.VMEM((mix, width), bf16),
            pltpu.VMEM((width, width), bf16),
            pltpu.VMEM((pieces, lump, mix), bf16),
            pltpu.VMEM((2, 2, pieces, lump, mix), bf16),
            pltpu.VMEM((2, pairs, mix), bf16),
            pltpu.VMEM((pieces, 2, lump, mix), f32),
            pltpu.VMEM((2, pairs, mix), f32),
            pltpu.VMEM((2, chunks, size, mix), bf16),
            pltpu.VMEM((2, chunks, size, mix), f32),
            pltpu.VMEM((slots, size, mix), bf16),
            pltpu.VMEM((pairs, width), f32),
        ],
        compiler_params=pltpu.CompilerParams(collective_id=0, has_side_effects=True),
    )(
        pair_rows, in_gain.reshape(1, width), left_weight, right_weight,
        mid_gain.reshape(1, mix), out_weight, out_gate,
    )
    return out.reshape(rows, cols, width)


def shards(pair_rows, in_gain, left_weight, right_weight, mid_gain, out_weight, out_gate):
    ready = norm_channels(pair_rows.astype(jnp.float32), in_gain).astype(jnp.bfloat16)
    ready = lax.optimization_barrier(ready)
    left = jnp.einsum("ijc,cd->ijd", ready, left_weight, preferred_element_type=jnp.float32)
    right = jnp.einsum("ijc,cd->ijd", ready, right_weight, preferred_element_type=jnp.float32)
    left, right = left.astype(jnp.bfloat16), right.astype(jnp.bfloat16)
    count = pair_rows.shape[0] * lax.axis_size("first")
    left_lines, right_lines = (
        lax.all_to_all(left, "first", split_axis=2, concat_axis=0, tiled=True),
        lax.all_to_all(right, "first", split_axis=2, concat_axis=0, tiled=True),
    )
    strip = jnp.einsum(
        "kid,kjd->ijd",
        lax.all_gather(left_lines, "second", axis=1, tiled=True),
        right_lines,
        preferred_element_type=jnp.float32,
    )
    strip = (strip * count ** (-0.5)).astype(jnp.bfloat16)
    mixed = lax.all_to_all(strip, "first", split_axis=0, concat_axis=2, tiled=True)
    scaled = norm_channels(mixed.astype(jnp.float32), mid_gain).astype(jnp.bfloat16)
    scaled = lax.optimization_barrier(scaled)
    gate = jax.nn.sigmoid(
        jnp.einsum("ijc,cd->ijd", ready, out_gate, preferred_element_type=jnp.float32)
    )
    return (
        jnp.einsum("ijd,dc->ijc", scaled, out_weight, preferred_element_type=jnp.float32) * gate
    ).astype(jnp.bfloat16)


def solution(mesh):
    in_specs = (P("first", "second", None), P(), P(), P(), P(), P(), P())
    out_specs = P("first", "second", None)
    planes, lines = mesh.shape["first"] // 2, mesh.shape["second"]
    if planes == lines == 4:
        body = functools.partial(triangle, planes, lines)
    else:
        body = shards
    return jax.shard_map(body, mesh=mesh, in_specs=in_specs, out_specs=out_specs, check_vma=False)
```

```python
import functools

import jax
import jax.numpy as jnp
from jax import lax
from jax.experimental import pallas as pl
from jax.experimental.pallas import tpu as pltpu
from jax.sharding import PartitionSpec as P

MESH = pl.DeviceIdType.MESH


def norm_channels(values, channel_gain):
    centred = values - jnp.mean(values, axis=-1, keepdims=True)
    return (
        centred
        * lax.rsqrt(jnp.mean(centred * centred, axis=-1, keepdims=True) + 1e-05)
        * channel_gain
    )


def dot(a, b):
    return jnp.dot(a, b, preferred_element_type=jnp.float32)


PIECE = 8
CHUNK = 2
DIRECT = 2


def other(index):
    return index + 1 - 2 * lax.rem(index, 2)


def centre(values, channel_gain):
    centred = values - jnp.mean(values, axis=-1, keepdims=True)
    scale = lax.rsqrt(jnp.mean(centred * centred, axis=-1, keepdims=True) + 1e-05)
    return (centred * channel_gain).astype(jnp.bfloat16), scale


def triangle_kernel(rows, cols, planes, lines, *refs):
    pieces, chunks = cols // PIECE, cols // CHUNK
    pl.run_scoped(
        functools.partial(triangle_steps, rows, cols, planes, lines, *refs),
        pltpu.SemaphoreType.DMA((6 + pieces,)),
        pltpu.SemaphoreType.DMA((lines, pieces)),
        pltpu.SemaphoreType.DMA((2, 2, pieces)),
        pltpu.SemaphoreType.DMA,
        pltpu.SemaphoreType.DMA,
        pltpu.SemaphoreType.DMA((2, chunks)),
        pltpu.SemaphoreType.DMA((2 * chunks + 4 * (chunks // 2),)),
        pltpu.SemaphoreType.REGULAR,
        pltpu.SemaphoreType.REGULAR,
        pltpu.SemaphoreType.REGULAR,
        pltpu.SemaphoreType.REGULAR,
    )


def triangle_steps(
    rows, cols, planes, lines,
    x_hbm, in_gain_hbm, left_w_hbm, right_w_hbm, mid_gain_hbm, out_w_hbm, gate_w_hbm,
    out_ref,
    x_ref, in_gain_ref, left_w_ref, right_w_ref, mid_gain_ref, out_w_ref, gate_w_ref,
    lsend, lrecv, rboth, left32, right32, psend, part32, inbox, gate,
    in_sem, lsend_sem, lrecv_sem, rsend_sem, rrecv_sem, psend_sem, inbox_sem, go_sem, across_sem, cross_sem, near_sem,
):
    first, second = lax.axis_index("first"), lax.axis_index("second")
    z, core = lax.div(first, 2), lax.rem(first, 2)
    pieces, chunks = cols // PIECE, cols // CHUNK
    per_piece, per_core = PIECE // CHUNK, chunks // 2
    lump, size = rows * PIECE, CHUNK * cols
    half = planes // 2
    upper, side, parity = lax.div(z, half), lax.div(second, half), lax.rem(second, 2)
    near_z = other(z)
    inner = lax.rem(z, 2) != upper
    outer = jnp.logical_not(inner)
    crossing = core == 1
    level = core == 0
    target_side = jnp.where(crossing, 1 - upper, upper)
    planes_of = [half * target_side + lax.rem(parity + u, 2) for u in range(2)]
    from_own = target_side == side
    is_own = [jnp.logical_and(level, planes_of[u] == z) for u in range(2)]
    is_near = [jnp.logical_and(level, planes_of[u] != z) for u in range(2)]
    x_second, y_second = other(second), lax.rem(second + half, lines)
    xy_second = other(y_second)
    cross_z = 2 * lax.rem(upper + 1, 2) + lax.rem(upper + 1 + 1, 2)

    def device(z_at, core_at, second_at):
        return {"first": 2 * z_at + core_at, "second": second_at}

    scope = jax.named_scope
    barrier = pltpu.get_barrier_semaphore()

    def greet(z_at, core_at, second_at):
        pl.semaphore_signal(
            barrier, inc=1, device_id=device(z_at, core_at, second_at), device_id_type=MESH
        )

    target = lax.rem(side + upper, 2)
    early = jnp.logical_and(crossing, jnp.logical_and(inner, upper == 0))
    even = lax.rem(z, 2) == 0
    far_target = jnp.logical_and(jnp.logical_and(crossing, upper == 0), lax.rem(z, 2) != parity)
    last_column = second == lines - 1
    slow_column = second == half

    with scope("sig"):
        greet(z, 1 - core, second)

        @pl.when(far_target)
        def _():
            greet(planes - 1, 1, second)

        for c in range(2):

            @pl.when(from_own)
            def _():
                greet(z, c, x_second)

            @pl.when(jnp.logical_not(from_own))
            def _():
                greet(z, c, y_second)

        @pl.when(jnp.logical_and(crossing, jnp.logical_not(last_column)))
        def _():
            greet(z, 1, x_second)

        @pl.when(jnp.logical_and(second == 0, jnp.logical_not(from_own)))
        def _():
            for c in range(2):
                greet(z, c, xy_second)

        @pl.when(even)
        def _():
            greet(near_z, 0, second)

            @pl.when(level)
            def _():
                for c in range(2):
                    greet(near_z, c, second)

            @pl.when(crossing)
            def _():
                greet(near_z, 1, second)

        @pl.when(upper == 0)
        def _():
            greet(cross_z, 1, second)

        @pl.when(early)
        def _():
            for dz in range(half):
                for c in range(2):
                    greet(half + dz, c, second)

    loads = [
        pltpu.make_async_copy(src, dst, in_sem.at[n])
        for n, (src, dst) in enumerate((
            (in_gain_hbm, in_gain_ref), (left_w_hbm, left_w_ref),
            *((x_hbm.at[:, pl.ds(c * PIECE, PIECE), :], x_ref.at[c]) for c in range(pieces)),
            (right_w_hbm, right_w_ref),
            (gate_w_hbm, gate_w_ref), (mid_gain_hbm, mid_gain_ref), (out_w_hbm, out_w_ref),
        ))
    ]
    for load in loads:
        load.start()
    def meet():
        signals = (
            3
            + jnp.where(even, 0, 1 + jnp.where(level, 2, 1))
            + jnp.where(jnp.logical_and(crossing, z == half), 2 * half, 0)
            + jnp.where(jnp.logical_and(crossing, z == planes - 1), 1, 0)
            + jnp.where(last_column, 1, 0)
            + jnp.where(jnp.logical_and(crossing, second != half), 1, 0)
            + upper
        )
        pl.semaphore_wait(barrier, signals.astype(jnp.int32))

        def answer(semaphore, z_at, core_at, second_at):
            pl.semaphore_signal(
                semaphore, inc=1, device_id=device(z_at, core_at, second_at), device_id_type=MESH
            )

        @pl.when(jnp.logical_and(crossing, second != half))
        def _():
            answer(across_sem, z, 1, x_second)

        @pl.when(jnp.logical_not(even))
        def _():
            answer(near_sem, near_z, 0, second)

        @pl.when(early)
        def _():
            answer(near_sem, near_z, 1, second)

        @pl.when(upper == 1)
        def _():
            answer(cross_sem, cross_z, 1, second)

    with scope("bar"):
        pl.when(last_column)(meet)

    def left_copy(t, c):
        return pltpu.make_async_remote_copy(
            src_ref=lsend.at[c],
            dst_ref=lrecv.at[t % 2, core, c],
            send_sem=lsend_sem.at[t, c],
            recv_sem=lrecv_sem.at[t % 2, core, c],
            device_id=device(z, target, (second, x_second, y_second, xy_second)[t]),
            device_id_type=MESH,
        )

    with scope("load"):
        loads[0].wait()
        loads[1].wait()

    def send_left(c):
        for t in (2, 1):
            left_copy(t, c).start()

        @pl.when(target != core)
        def _():
            left_copy(0, c).start()

    ready, scales = [], []
    for c in range(pieces):
        with scope(f"left{c}"):
            loads[2 + c].wait()
            x = x_ref[c].astype(jnp.float32).reshape(lump, x_ref.shape[-1])
            for list_of, value in zip((ready, scales), centre(x, in_gain_ref[...])):
                list_of.append(value)
            lsend[c] = (dot(ready[c], left_w_ref[...]) * scales[c]).astype(jnp.bfloat16)
        if c == 0:
            with scope("bar0"):
                pl.when(side == 0)(meet)

        @pl.when(jnp.logical_not(slow_column))
        def _():
            send_left(c)

    with scope("right"):
        loads[pieces + 2].wait()
        ready, scales = (jnp.concatenate(list_of, axis=0) for list_of in (ready, scales))
        right = (dot(ready, right_w_ref[...]) * scales).astype(jnp.bfloat16)
        rboth[core] = right
    with scope("bar2"):

        @pl.when(slow_column)
        def _():
            meet()
            for c in range(pieces):
                send_left(c)

    right_copy = pltpu.make_async_remote_copy(
        src_ref=rboth.at[core],
        dst_ref=rboth.at[core],
        send_sem=rsend_sem,
        recv_sem=rrecv_sem,
        device_id=device(z, 1 - core, second),
        device_id_type=MESH,
    )
    right_copy.start()
    with scope("across"):
        @pl.when(jnp.logical_not(last_column))
        def _():
            pl.semaphore_wait(across_sem, 1)

            @pl.when(crossing)
            def _():
                pl.semaphore_signal(
                    across_sem, inc=1, device_id=device(z, 0, second), device_id_type=MESH
                )

        for c in range(pieces):
            left_copy(3, c).start()
    with scope("gate"):
        loads[pieces + 3].wait()
        gates = jax.nn.sigmoid(dot(ready, gate_w_ref[...]) * scales)
        for c in range(pieces):
            for k in range(rows):
                at = c * lump + k * PIECE
                gate[k * cols + c * PIECE : k * cols + (c + 1) * PIECE, :] = gates[at : at + PIECE, :]
        loads[pieces + 4].wait()
        loads[pieces + 5].wait()

    with scope("rwait"):
        right_copy.wait_recv()
    with scope("r32"):
        for q in range(2):
            right32[q] = rboth[q].astype(jnp.float32)

    def send(j, n, slot, to):
        return pltpu.make_async_remote_copy(
            src_ref=psend.at[j, n],
            dst_ref=inbox.at[slot],
            send_sem=psend_sem.at[j, n],
            recv_sem=inbox_sem.at[slot],
            device_id=to,
            device_id_type=MESH,
        )

    near_at, cross_at, own_at, far_at = (2 * chunks + n * per_core for n in range(4))
    descending = jnp.logical_and(crossing, upper == 1)

    def waits(j, n):
        return j == 0 and n >= per_core

    def skips(j, n):
        return j == 1 and n >= chunks - DIRECT

    near_early = jnp.logical_and(upper == side, parity != lax.rem(z, 2))
    held_back = outer

    def relay_copy(j, n):
        return send(j, n, j * chunks + n, device(near_z, 1, second))

    def far_copy(j, n):
        return send(j, n, far_at + n % per_core, device(planes_of[j], 1, second))

    def near_copy(j, n):
        return send(j, n, near_at + n % per_core, device(near_z, n // per_core, second))

    def cross_copy(j, n):
        return send(j, n, cross_at + n % per_core, device(planes_of[j], n // per_core, second))

    def own_copy(j, n):
        return send(j, n, own_at + n % per_core, device(z, 1, second))

    def block(j, c):
        with scope(f"wl{j}{c}"):
            for q in range(2):
                mine = jnp.logical_and(from_own, core == q) if j == 0 else None

                def arrived():
                    pltpu.make_async_remote_copy(
                        src_ref=lsend.at[c],
                        dst_ref=lrecv.at[j, q, c],
                        send_sem=lsend_sem.at[0, c],
                        recv_sem=lrecv_sem.at[j, q, c],
                        device_id=device(z, 1 - core, second),
                        device_id_type=MESH,
                    ).wait_recv()
                    left32[c, q] = lrecv[j, q, c].astype(jnp.float32)

                if j:
                    arrived()
                else:
                    pl.when(jnp.logical_not(mine))(arrived)

                    @pl.when(mine)
                    def _():
                        left32[c, q] = lsend[c].astype(jnp.float32)

        with scope(f"block{j}{c}"):
            for part in range(per_piece):
                n = c * per_piece + part
                sums = tuple(jnp.zeros((cols, x_ref.shape[-1]), jnp.float32) for _ in range(CHUNK))
                for q in range(2):

                    def body(k, sums):
                        at = pl.multiple_of(k * PIECE, PIECE)
                        r = jnp.concatenate(
                            [right32[q, pl.ds(p * lump + at, PIECE), :] for p in range(pieces)], axis=0
                        )
                        return tuple(
                            total + left32[c, q, pl.ds(at + part * CHUNK + i, 1), :] * r
                            for i, total in enumerate(sums)
                        )

                    sums = lax.fori_loop(0, rows, body, sums, unroll=True)
                total = jnp.concatenate(sums, axis=0)

                @pl.when(jnp.logical_and(crossing, inner))
                def _():
                    part32[j, n] = total

                psend[j, n] = total.astype(jnp.bfloat16)

                sends = jnp.logical_and(crossing, outer)
                if skips(j, n):
                    sends = jnp.logical_and(sends, upper == 0)
                if waits(j, n):
                    sends = jnp.logical_and(sends, parity == 0)

                @pl.when(sends)
                def _():
                    relay_copy(j, n).start()

                if skips(j, n):

                    @pl.when(jnp.logical_and(descending, outer))
                    def _():
                        far_copy(j, n).start()

                    @pl.when(jnp.logical_and(descending, inner))
                    def _():
                        cross_copy(j, n).start()

                @pl.when(is_own[j])
                def _():
                    if n < per_core:
                        inbox[own_at + n] = psend[j, n]
                    else:
                        own_copy(j, n).start()

                @pl.when(jnp.logical_and(is_near[j], jnp.logical_not(held_back)))
                def _():
                    near_copy(j, n).start()

    with scope("nearbar"):

        @pl.when(jnp.logical_and(even, level))
        def _():
            pl.semaphore_wait(near_sem, 2)

        @pl.when(jnp.logical_and(z == 0, crossing))
        def _():
            pl.semaphore_wait(near_sem, 1)

    def near_after_go():
        pl.semaphore_wait(go_sem, 1)
        for n in range(chunks):
            near_copy(0, n).start()

    for j in range(2):
        for c in range(pieces):
            block(j, c)
        if j == 0:
            with scope("held0"):

                @pl.when(jnp.logical_and(level, jnp.logical_and(held_back, is_near[0])))
                def _():
                    pl.when(jnp.logical_not(from_own))(near_after_go)


    by_plane = [(j, n) for j in range(2) for n in range(chunks)]
    by_need = sorted(by_plane, key=lambda at: waits(*at))
    with scope("late"):

        @pl.when(jnp.logical_and(jnp.logical_and(crossing, outer), parity == 1))
        def _():
            for j, n in by_plane:
                if waits(j, n):
                    relay_copy(j, n).start()

    with scope("relay"):

        @pl.when(early)
        def _():
            pl.semaphore_wait(cross_sem, 2 * half)

        @pl.when(jnp.logical_and(crossing, inner))
        def _():
            def relay(j, n):
                relay_copy(j, n).wait_recv()
                total = part32[j, n] + inbox[j * chunks + n].astype(jnp.float32)
                psend[j, n] = total.astype(jnp.bfloat16)
                cross_copy(j, n).start()

            def relay_all(order):
                for j, n in order:
                    if skips(j, n):
                        pl.when(upper == 0)(functools.partial(relay, j, n))
                    else:
                        relay(j, n)

            pl.when(parity == 0)(lambda: relay_all(by_plane))
            pl.when(parity == 1)(lambda: relay_all(by_need))

    cuts = (by_plane, 2 * chunks - chunks // 4), (by_need, 2 * chunks - per_core)

    def wait_sent(order):
        for j, n in order:
            near_copy(j, n).wait_send()

    with scope("held"):

        @pl.when(held_back)
        def _():
            @pl.when(crossing)
            def _():
                for odd, (order, cut) in enumerate(cuts):
                    pl.when(parity == odd)(functools.partial(wait_sent, order[:cut]))
                pl.semaphore_signal(go_sem, inc=1, device_id=device(z, 0, second), device_id_type=MESH)

            @pl.when(jnp.logical_and(level, is_near[0]))
            def _():
                pl.when(from_own)(near_after_go)

            @pl.when(jnp.logical_and(level, is_near[1]))
            def _():
                pl.semaphore_wait(go_sem, 1)
                for n in range(chunks):
                    near_copy(1, n).start()

    count = rows * 2 * planes
    with scope("drain"):
        for t in (1, 2, 3):
            for c in range(pieces):
                left_copy(t, c).wait_send()

        @pl.when(target != core)
        def _():
            for c in range(pieces):
                left_copy(0, c).wait_send()

        right_copy.wait_send()

        @pl.when(crossing)
        def _():
            for odd, (order, cut) in enumerate(cuts):

                @pl.when(parity == odd)
                def _():
                    wait_sent(order[cut:])
                    pl.when(jnp.logical_not(held_back))(functools.partial(wait_sent, order[:cut]))

    def drain_level():
        for j, n in by_plane:
            if n < per_core:

                @pl.when(is_near[j])
                def _():
                    near_copy(j, n).wait_send()

            else:
                near_copy(j, n).wait_send()

    pl.when(jnp.logical_and(level, jnp.logical_not(held_back)))(drain_level)
    for c in range(per_core):
        with scope(f"own{c}"):

            @pl.when(crossing)
            def _():
                own_copy(0, c).wait_recv()

        with scope(f"near{c}"):
            near_copy(0, c).wait_recv()
    with scope("sum"):
        for c in range(per_core):
            part32[0, c] = inbox[own_at + c].astype(jnp.float32) + inbox[near_at + c].astype(jnp.float32)
    with scope("cross"):
        for c in range(per_core):
            cross_copy(0, c).wait_recv()
    with scope("far"):

        @pl.when(far_target)
        def _():
            for c in range(per_core - DIRECT, per_core):
                part32[0, c] = part32[0, c] + inbox[cross_at + c].astype(jnp.float32)
                send(0, c, far_at + c, device(near_z, 0, second)).wait_recv()

    last_at = [
        (jnp.where(far_target, far_at, cross_at) if c >= per_core - DIRECT else cross_at) + c
        for c in range(per_core)
    ]
    with scope("final"):
        total = jnp.concatenate(
            [part32[0, c] + inbox[last_at[c]].astype(jnp.float32) for c in range(per_core)], axis=0
        )
        mixed = (total * count ** (-0.5)).astype(jnp.bfloat16)
        scaled, scale = centre(mixed.astype(jnp.float32), mid_gain_ref[...])
        out_ref[...] = (dot(scaled, out_w_ref[...]) * (gate[...] * scale)).astype(jnp.bfloat16)

    pl.when(jnp.logical_and(level, held_back))(drain_level)


def triangle(planes, lines, pair_rows, in_gain, left_weight, right_weight, mid_gain, out_weight, out_gate):
    rows, cols, width = pair_rows.shape
    mix = left_weight.shape[1]
    pairs, pieces, chunks, size = rows * cols, cols // PIECE, cols // CHUNK, CHUNK * cols
    lump = rows * PIECE
    slots = 2 * chunks + 4 * (chunks // 2)
    anywhere = pl.BlockSpec(memory_space=pl.ANY)
    bf16, f32 = jnp.bfloat16, jnp.float32
    out = pl.pallas_call(
        functools.partial(triangle_kernel, rows, cols, planes, lines),
        out_shape=pltpu.VMEM((pairs, width), bf16),
        in_specs=[anywhere] * 7,
        out_specs=pl.BlockSpec(memory_space=pltpu.VMEM),
        scratch_shapes=[
            pltpu.VMEM((pieces, rows, PIECE, width), bf16),
            pltpu.VMEM((1, width), f32),
            pltpu.VMEM((width, mix), bf16),
            pltpu.VMEM((width, mix), bf16),
            pltpu.VMEM((1, mix), f32),
            pltpu.VMEM((mix, width), bf16),
            pltpu.VMEM((width, width), bf16),
            pltpu.VMEM((pieces, lump, mix), bf16),
            pltpu.VMEM((2, 2, pieces, lump, mix), bf16),
            pltpu.VMEM((2, pairs, mix), bf16),
            pltpu.VMEM((pieces, 2, lump, mix), f32),
            pltpu.VMEM((2, pairs, mix), f32),
            pltpu.VMEM((2, chunks, size, mix), bf16),
            pltpu.VMEM((2, chunks, size, mix), f32),
            pltpu.VMEM((slots, size, mix), bf16),
            pltpu.VMEM((pairs, width), f32),
        ],
        compiler_params=pltpu.CompilerParams(collective_id=0, has_side_effects=True),
    )(
        pair_rows, in_gain.reshape(1, width), left_weight, right_weight,
        mid_gain.reshape(1, mix), out_weight, out_gate,
    )
    return out.reshape(rows, cols, width)


def shards(pair_rows, in_gain, left_weight, right_weight, mid_gain, out_weight, out_gate):
    ready = norm_channels(pair_rows.astype(jnp.float32), in_gain).astype(jnp.bfloat16)
    ready = lax.optimization_barrier(ready)
    left = jnp.einsum("ijc,cd->ijd", ready, left_weight, preferred_element_type=jnp.float32)
    right = jnp.einsum("ijc,cd->ijd", ready, right_weight, preferred_element_type=jnp.float32)
    left, right = left.astype(jnp.bfloat16), right.astype(jnp.bfloat16)
    count = pair_rows.shape[0] * lax.axis_size("first")
    left_lines, right_lines = (
        lax.all_to_all(left, "first", split_axis=2, concat_axis=0, tiled=True),
        lax.all_to_all(right, "first", split_axis=2, concat_axis=0, tiled=True),
    )
    strip = jnp.einsum(
        "kid,kjd->ijd",
        lax.all_gather(left_lines, "second", axis=1, tiled=True),
        right_lines,
        preferred_element_type=jnp.float32,
    )
    strip = (strip * count ** (-0.5)).astype(jnp.bfloat16)
    mixed = lax.all_to_all(strip, "first", split_axis=0, concat_axis=2, tiled=True)
    scaled = norm_channels(mixed.astype(jnp.float32), mid_gain).astype(jnp.bfloat16)
    scaled = lax.optimization_barrier(scaled)
    gate = jax.nn.sigmoid(
        jnp.einsum("ijc,cd->ijd", ready, out_gate, preferred_element_type=jnp.float32)
    )
    return (
        jnp.einsum("ijd,dc->ijc", scaled, out_weight, preferred_element_type=jnp.float32) * gate
    ).astype(jnp.bfloat16)


def solution(mesh):
    in_specs = (P("first", "second", None), P(), P(), P(), P(), P(), P())
    out_specs = P("first", "second", None)
    planes, lines = mesh.shape["first"] // 2, mesh.shape["second"]
    if planes == lines == 4:
        body = functools.partial(triangle, planes, lines)
    else:
        body = shards
    return jax.shard_map(body, mesh=mesh, in_specs=in_specs, out_specs=out_specs, check_vma=False)
```

```python
import functools

import jax
import jax.numpy as jnp
from jax import lax
from jax.experimental import pallas as pl
from jax.experimental.pallas import tpu as pltpu
from jax.sharding import PartitionSpec as P

MESH = pl.DeviceIdType.MESH


def norm_channels(values, channel_gain):
    centred = values - jnp.mean(values, axis=-1, keepdims=True)
    return (
        centred
        * lax.rsqrt(jnp.mean(centred * centred, axis=-1, keepdims=True) + 1e-05)
        * channel_gain
    )


def dot(a, b):
    return jnp.dot(a, b, preferred_element_type=jnp.float32)


PIECE = 8
CHUNK = 2
DIRECT = 2


def other(index):
    return index + 1 - 2 * lax.rem(index, 2)


def centre(values, channel_gain):
    centred = values - jnp.mean(values, axis=-1, keepdims=True)
    scale = lax.rsqrt(jnp.mean(centred * centred, axis=-1, keepdims=True) + 1e-05)
    return (centred * channel_gain).astype(jnp.bfloat16), scale


def triangle_kernel(rows, cols, planes, lines, *refs):
    pieces, chunks = cols // PIECE, cols // CHUNK
    pl.run_scoped(
        functools.partial(triangle_steps, rows, cols, planes, lines, *refs),
        pltpu.SemaphoreType.DMA((6 + pieces,)),
        pltpu.SemaphoreType.DMA((lines, pieces)),
        pltpu.SemaphoreType.DMA((2, 2, pieces)),
        pltpu.SemaphoreType.DMA,
        pltpu.SemaphoreType.DMA,
        pltpu.SemaphoreType.DMA((2, chunks)),
        pltpu.SemaphoreType.DMA((2 * chunks + 4 * (chunks // 2),)),
        pltpu.SemaphoreType.REGULAR,
        pltpu.SemaphoreType.REGULAR,
        pltpu.SemaphoreType.REGULAR,
        pltpu.SemaphoreType.REGULAR,
    )


def triangle_steps(
    rows, cols, planes, lines,
    x_hbm, in_gain_hbm, left_w_hbm, right_w_hbm, mid_gain_hbm, out_w_hbm, gate_w_hbm,
    out_ref,
    x_ref, in_gain_ref, left_w_ref, right_w_ref, mid_gain_ref, out_w_ref, gate_w_ref,
    lsend, lrecv, rboth, left32, right32, psend, part32, inbox, gate,
    in_sem, lsend_sem, lrecv_sem, rsend_sem, rrecv_sem, psend_sem, inbox_sem, go_sem, across_sem, cross_sem, near_sem,
):
    first, second = lax.axis_index("first"), lax.axis_index("second")
    z, core = lax.div(first, 2), lax.rem(first, 2)
    pieces, chunks = cols // PIECE, cols // CHUNK
    per_piece, per_core = PIECE // CHUNK, chunks // 2
    lump, size = rows * PIECE, CHUNK * cols
    half = planes // 2
    upper, side, parity = lax.div(z, half), lax.div(second, half), lax.rem(second, 2)
    near_z = other(z)
    inner = lax.rem(z, 2) != upper
    outer = jnp.logical_not(inner)
    crossing = core == 1
    level = core == 0
    target_side = jnp.where(crossing, 1 - upper, upper)
    planes_of = [half * target_side + lax.rem(parity + u, 2) for u in range(2)]
    from_own = target_side == side
    is_own = [jnp.logical_and(level, planes_of[u] == z) for u in range(2)]
    is_near = [jnp.logical_and(level, planes_of[u] != z) for u in range(2)]
    x_second, y_second = other(second), lax.rem(second + half, lines)
    xy_second = other(y_second)
    cross_z = 2 * lax.rem(upper + 1, 2) + lax.rem(upper + 1 + 1, 2)

    def device(z_at, core_at, second_at):
        return {"first": 2 * z_at + core_at, "second": second_at}

    scope = jax.named_scope
    barrier = pltpu.get_barrier_semaphore()

    def greet(z_at, core_at, second_at):
        pl.semaphore_signal(
            barrier, inc=1, device_id=device(z_at, core_at, second_at), device_id_type=MESH
        )

    target = lax.rem(side + upper, 2)
    early = jnp.logical_and(crossing, jnp.logical_and(inner, upper == 0))
    even = lax.rem(z, 2) == 0
    far_target = jnp.logical_and(jnp.logical_and(crossing, upper == 0), lax.rem(z, 2) != parity)
    last_column = second == lines - 1
    slow_column = second == half

    with scope("sig"):
        greet(z, 1 - core, second)

        @pl.when(far_target)
        def _():
            greet(planes - 1, 1, second)

        for c in range(2):

            @pl.when(from_own)
            def _():
                greet(z, c, x_second)

            @pl.when(jnp.logical_not(from_own))
            def _():
                greet(z, c, y_second)

        @pl.when(jnp.logical_and(crossing, jnp.logical_not(last_column)))
        def _():
            greet(z, 1, x_second)

        @pl.when(jnp.logical_and(second == 0, jnp.logical_not(from_own)))
        def _():
            for c in range(2):
                greet(z, c, xy_second)

        @pl.when(even)
        def _():
            greet(near_z, 0, second)

            @pl.when(level)
            def _():
                for c in range(2):
                    greet(near_z, c, second)

            @pl.when(crossing)
            def _():
                greet(near_z, 1, second)

        @pl.when(upper == 0)
        def _():
            greet(cross_z, 1, second)

        @pl.when(early)
        def _():
            for dz in range(half):
                for c in range(2):
                    greet(half + dz, c, second)

    loads = [
        pltpu.make_async_copy(src, dst, in_sem.at[n])
        for n, (src, dst) in enumerate((
            (in_gain_hbm, in_gain_ref), (left_w_hbm, left_w_ref),
            *((x_hbm.at[:, pl.ds(c * PIECE, PIECE), :], x_ref.at[c]) for c in range(pieces)),
            (right_w_hbm, right_w_ref),
            (gate_w_hbm, gate_w_ref), (mid_gain_hbm, mid_gain_ref), (out_w_hbm, out_w_ref),
        ))
    ]
    for load in loads:
        load.start()
    def meet():
        signals = (
            3
            + jnp.where(even, 0, 1 + jnp.where(level, 2, 1))
            + jnp.where(jnp.logical_and(crossing, z == half), 2 * half, 0)
            + jnp.where(jnp.logical_and(crossing, z == planes - 1), 1, 0)
            + jnp.where(last_column, 1, 0)
            + jnp.where(jnp.logical_and(crossing, second != half), 1, 0)
            + upper
        )
        pl.semaphore_wait(barrier, signals.astype(jnp.int32))

        def answer(semaphore, z_at, core_at, second_at):
            pl.semaphore_signal(
                semaphore, inc=1, device_id=device(z_at, core_at, second_at), device_id_type=MESH
            )

        @pl.when(jnp.logical_and(crossing, second != half))
        def _():
            answer(across_sem, z, 1, x_second)

        @pl.when(jnp.logical_not(even))
        def _():
            answer(near_sem, near_z, 0, second)

        @pl.when(early)
        def _():
            answer(near_sem, near_z, 1, second)

        @pl.when(upper == 1)
        def _():
            answer(cross_sem, cross_z, 1, second)

    with scope("bar"):
        pl.when(last_column)(meet)

    def left_copy(t, c):
        return pltpu.make_async_remote_copy(
            src_ref=lsend.at[c],
            dst_ref=lrecv.at[t % 2, core, c],
            send_sem=lsend_sem.at[t, c],
            recv_sem=lrecv_sem.at[t % 2, core, c],
            device_id=device(z, target, (second, x_second, y_second, xy_second)[t]),
            device_id_type=MESH,
        )

    with scope("load"):
        loads[0].wait()
        loads[1].wait()

    def send_left(c):
        for t in (2, 1):
            left_copy(t, c).start()

        @pl.when(target != core)
        def _():
            left_copy(0, c).start()

    ready, scales = [], []
    for c in range(pieces):
        with scope(f"left{c}"):
            loads[2 + c].wait()
            x = x_ref[c].astype(jnp.float32).reshape(lump, x_ref.shape[-1])
            for list_of, value in zip((ready, scales), centre(x, in_gain_ref[...])):
                list_of.append(value)
            lsend[c] = (dot(ready[c], left_w_ref[...]) * scales[c]).astype(jnp.bfloat16)
        if c == 0:
            with scope("bar0"):
                pl.when(side == 0)(meet)

        @pl.when(jnp.logical_not(slow_column))
        def _():
            send_left(c)

    with scope("right"):
        loads[pieces + 2].wait()
        ready, scales = (jnp.concatenate(list_of, axis=0) for list_of in (ready, scales))
        right = (dot(ready, right_w_ref[...]) * scales).astype(jnp.bfloat16)
        rboth[core] = right
    with scope("bar2"):

        @pl.when(slow_column)
        def _():
            meet()
            for c in range(pieces):
                send_left(c)

    right_copy = pltpu.make_async_remote_copy(
        src_ref=rboth.at[core],
        dst_ref=rboth.at[core],
        send_sem=rsend_sem,
        recv_sem=rrecv_sem,
        device_id=device(z, 1 - core, second),
        device_id_type=MESH,
    )
    right_copy.start()
    with scope("across"):
        @pl.when(jnp.logical_not(last_column))
        def _():
            pl.semaphore_wait(across_sem, 1)

            @pl.when(crossing)
            def _():
                pl.semaphore_signal(
                    across_sem, inc=1, device_id=device(z, 0, second), device_id_type=MESH
                )

        for c in range(pieces):
            left_copy(3, c).start()
    with scope("gate"):
        loads[pieces + 3].wait()
        gates = jax.nn.sigmoid(dot(ready, gate_w_ref[...]) * scales)
        for c in range(pieces):
            for k in range(rows):
                at = c * lump + k * PIECE
                gate[k * cols + c * PIECE : k * cols + (c + 1) * PIECE, :] = gates[at : at + PIECE, :]
        loads[pieces + 4].wait()
        loads[pieces + 5].wait()

    with scope("rwait"):
        right_copy.wait_recv()
    with scope("r32"):
        for q in range(2):
            right32[q] = rboth[q].astype(jnp.float32)

    def send(j, n, slot, to):
        return pltpu.make_async_remote_copy(
            src_ref=psend.at[j, n],
            dst_ref=inbox.at[slot],
            send_sem=psend_sem.at[j, n],
            recv_sem=inbox_sem.at[slot],
            device_id=to,
            device_id_type=MESH,
        )

    near_at, cross_at, own_at, far_at = (2 * chunks + n * per_core for n in range(4))
    descending = jnp.logical_and(crossing, upper == 1)

    def waits(j, n):
        return j == 0 and n >= per_core

    def skips(j, n):
        return j == 1 and n >= chunks - DIRECT

    near_early = jnp.logical_and(upper == side, parity != lax.rem(z, 2))
    held_back = outer

    def relay_copy(j, n):
        return send(j, n, j * chunks + n, device(near_z, 1, second))

    def far_copy(j, n):
        return send(j, n, far_at + n % per_core, device(planes_of[j], 1, second))

    def near_copy(j, n):
        return send(j, n, near_at + n % per_core, device(near_z, n // per_core, second))

    def cross_copy(j, n):
        return send(j, n, cross_at + n % per_core, device(planes_of[j], n // per_core, second))

    def own_copy(j, n):
        return send(j, n, own_at + n % per_core, device(z, 1, second))

    def block(j, c):
        with scope(f"wl{j}{c}"):
            for q in range(2):
                mine = jnp.logical_and(from_own, core == q) if j == 0 else None

                def arrived():
                    pltpu.make_async_remote_copy(
                        src_ref=lsend.at[c],
                        dst_ref=lrecv.at[j, q, c],
                        send_sem=lsend_sem.at[0, c],
                        recv_sem=lrecv_sem.at[j, q, c],
                        device_id=device(z, 1 - core, second),
                        device_id_type=MESH,
                    ).wait_recv()
                    left32[c, q] = lrecv[j, q, c].astype(jnp.float32)

                if j:
                    arrived()
                else:
                    pl.when(jnp.logical_not(mine))(arrived)

                    @pl.when(mine)
                    def _():
                        left32[c, q] = lsend[c].astype(jnp.float32)

        with scope(f"block{j}{c}"):
            for part in range(per_piece):
                n = c * per_piece + part
                sums = tuple(jnp.zeros((cols, x_ref.shape[-1]), jnp.float32) for _ in range(CHUNK))
                for q in range(2):

                    def body(k, sums):
                        at = pl.multiple_of(k * PIECE, PIECE)
                        r = jnp.concatenate(
                            [right32[q, pl.ds(p * lump + at, PIECE), :] for p in range(pieces)], axis=0
                        )
                        return tuple(
                            total + left32[c, q, pl.ds(at + part * CHUNK + i, 1), :] * r
                            for i, total in enumerate(sums)
                        )

                    sums = lax.fori_loop(0, rows, body, sums, unroll=True)
                total = jnp.concatenate(sums, axis=0)

                @pl.when(jnp.logical_and(crossing, inner))
                def _():
                    part32[j, n] = total

                psend[j, n] = total.astype(jnp.bfloat16)

                sends = jnp.logical_and(crossing, outer)
                if skips(j, n):
                    sends = jnp.logical_and(sends, upper == 0)
                if waits(j, n):
                    sends = jnp.logical_and(sends, parity == 0)

                @pl.when(sends)
                def _():
                    relay_copy(j, n).start()

                if skips(j, n):

                    @pl.when(jnp.logical_and(descending, outer))
                    def _():
                        far_copy(j, n).start()

                    @pl.when(jnp.logical_and(descending, inner))
                    def _():
                        cross_copy(j, n).start()

                @pl.when(is_own[j])
                def _():
                    if n < per_core:
                        inbox[own_at + n] = psend[j, n]
                    else:
                        own_copy(j, n).start()

                @pl.when(jnp.logical_and(is_near[j], jnp.logical_not(held_back)))
                def _():
                    near_copy(j, n).start()

    with scope("nearbar"):

        @pl.when(jnp.logical_and(even, level))
        def _():
            pl.semaphore_wait(near_sem, 2)

        @pl.when(jnp.logical_and(z == 0, crossing))
        def _():
            pl.semaphore_wait(near_sem, 1)

    def near_after_go():
        pl.semaphore_wait(go_sem, 1)
        for n in range(chunks):
            near_copy(0, n).start()

    for j in range(2):
        for c in range(pieces):
            block(j, c)
        if j == 0:
            with scope("held0"):

                @pl.when(jnp.logical_and(level, jnp.logical_and(held_back, is_near[0])))
                def _():
                    pl.when(jnp.logical_not(from_own))(near_after_go)


    by_plane = [(j, n) for j in range(2) for n in range(chunks)]
    by_need = sorted(by_plane, key=lambda at: waits(*at))
    with scope("late"):

        @pl.when(jnp.logical_and(jnp.logical_and(crossing, outer), parity == 1))
        def _():
            for j, n in by_plane:
                if waits(j, n):
                    relay_copy(j, n).start()

    with scope("relay"):

        @pl.when(early)
        def _():
            pl.semaphore_wait(cross_sem, 2 * half)

        @pl.when(jnp.logical_and(crossing, inner))
        def _():
            def relay(j, n):
                relay_copy(j, n).wait_recv()
                total = part32[j, n] + inbox[j * chunks + n].astype(jnp.float32)
                psend[j, n] = total.astype(jnp.bfloat16)
                cross_copy(j, n).start()

            def relay_all(order):
                for j, n in order:
                    if skips(j, n):
                        pl.when(upper == 0)(functools.partial(relay, j, n))
                    else:
                        relay(j, n)

            pl.when(parity == 0)(lambda: relay_all(by_plane))
            pl.when(parity == 1)(lambda: relay_all(by_need))

    cuts = (by_plane, 2 * chunks - chunks // 4), (by_need, 2 * chunks - per_core - 3)

    def wait_sent(order):
        for j, n in order:
            near_copy(j, n).wait_send()

    with scope("held"):

        @pl.when(held_back)
        def _():
            @pl.when(crossing)
            def _():
                for odd, (order, cut) in enumerate(cuts):
                    pl.when(parity == odd)(functools.partial(wait_sent, order[:cut]))
                pl.semaphore_signal(go_sem, inc=1, device_id=device(z, 0, second), device_id_type=MESH)

            @pl.when(jnp.logical_and(level, is_near[0]))
            def _():
                pl.when(from_own)(near_after_go)

            @pl.when(jnp.logical_and(level, is_near[1]))
            def _():
                pl.semaphore_wait(go_sem, 1)
                for n in range(chunks):
                    near_copy(1, n).start()

    count = rows * 2 * planes
    with scope("drain"):
        for t in (1, 2, 3):
            for c in range(pieces):
                left_copy(t, c).wait_send()

        @pl.when(target != core)
        def _():
            for c in range(pieces):
                left_copy(0, c).wait_send()

        right_copy.wait_send()

        @pl.when(crossing)
        def _():
            for odd, (order, cut) in enumerate(cuts):

                @pl.when(parity == odd)
                def _():
                    wait_sent(order[cut:])
                    pl.when(jnp.logical_not(held_back))(functools.partial(wait_sent, order[:cut]))

    def drain_level():
        for j, n in by_plane:
            if n < per_core:

                @pl.when(is_near[j])
                def _():
                    near_copy(j, n).wait_send()

            else:
                near_copy(j, n).wait_send()

    pl.when(jnp.logical_and(level, jnp.logical_not(held_back)))(drain_level)
    for c in range(per_core):
        with scope(f"own{c}"):

            @pl.when(crossing)
            def _():
                own_copy(0, c).wait_recv()

        with scope(f"near{c}"):
            near_copy(0, c).wait_recv()
    with scope("sum"):
        for c in range(per_core):
            part32[0, c] = inbox[own_at + c].astype(jnp.float32) + inbox[near_at + c].astype(jnp.float32)
    with scope("cross"):
        for c in range(per_core):
            cross_copy(0, c).wait_recv()
    with scope("far"):

        @pl.when(far_target)
        def _():
            for c in range(per_core - DIRECT, per_core):
                part32[0, c] = part32[0, c] + inbox[cross_at + c].astype(jnp.float32)
                send(0, c, far_at + c, device(near_z, 0, second)).wait_recv()

    last_at = [
        (jnp.where(far_target, far_at, cross_at) if c >= per_core - DIRECT else cross_at) + c
        for c in range(per_core)
    ]
    with scope("final"):
        total = jnp.concatenate(
            [part32[0, c] + inbox[last_at[c]].astype(jnp.float32) for c in range(per_core)], axis=0
        )
        mixed = (total * count ** (-0.5)).astype(jnp.bfloat16)
        scaled, scale = centre(mixed.astype(jnp.float32), mid_gain_ref[...])
        out_ref[...] = (dot(scaled, out_w_ref[...]) * (gate[...] * scale)).astype(jnp.bfloat16)

    pl.when(jnp.logical_and(level, held_back))(drain_level)


def triangle(planes, lines, pair_rows, in_gain, left_weight, right_weight, mid_gain, out_weight, out_gate):
    rows, cols, width = pair_rows.shape
    mix = left_weight.shape[1]
    pairs, pieces, chunks, size = rows * cols, cols // PIECE, cols // CHUNK, CHUNK * cols
    lump = rows * PIECE
    slots = 2 * chunks + 4 * (chunks // 2)
    anywhere = pl.BlockSpec(memory_space=pl.ANY)
    bf16, f32 = jnp.bfloat16, jnp.float32
    out = pl.pallas_call(
        functools.partial(triangle_kernel, rows, cols, planes, lines),
        out_shape=pltpu.VMEM((pairs, width), bf16),
        in_specs=[anywhere] * 7,
        out_specs=pl.BlockSpec(memory_space=pltpu.VMEM),
        scratch_shapes=[
            pltpu.VMEM((pieces, rows, PIECE, width), bf16),
            pltpu.VMEM((1, width), f32),
            pltpu.VMEM((width, mix), bf16),
            pltpu.VMEM((width, mix), bf16),
            pltpu.VMEM((1, mix), f32),
            pltpu.VMEM((mix, width), bf16),
            pltpu.VMEM((width, width), bf16),
            pltpu.VMEM((pieces, lump, mix), bf16),
            pltpu.VMEM((2, 2, pieces, lump, mix), bf16),
            pltpu.VMEM((2, pairs, mix), bf16),
            pltpu.VMEM((pieces, 2, lump, mix), f32),
            pltpu.VMEM((2, pairs, mix), f32),
            pltpu.VMEM((2, chunks, size, mix), bf16),
            pltpu.VMEM((2, chunks, size, mix), f32),
            pltpu.VMEM((slots, size, mix), bf16),
            pltpu.VMEM((pairs, width), f32),
        ],
        compiler_params=pltpu.CompilerParams(collective_id=0, has_side_effects=True),
    )(
        pair_rows, in_gain.reshape(1, width), left_weight, right_weight,
        mid_gain.reshape(1, mix), out_weight, out_gate,
    )
    return out.reshape(rows, cols, width)


def shards(pair_rows, in_gain, left_weight, right_weight, mid_gain, out_weight, out_gate):
    ready = norm_channels(pair_rows.astype(jnp.float32), in_gain).astype(jnp.bfloat16)
    ready = lax.optimization_barrier(ready)
    left = jnp.einsum("ijc,cd->ijd", ready, left_weight, preferred_element_type=jnp.float32)
    right = jnp.einsum("ijc,cd->ijd", ready, right_weight, preferred_element_type=jnp.float32)
    left, right = left.astype(jnp.bfloat16), right.astype(jnp.bfloat16)
    count = pair_rows.shape[0] * lax.axis_size("first")
    left_lines, right_lines = (
        lax.all_to_all(left, "first", split_axis=2, concat_axis=0, tiled=True),
        lax.all_to_all(right, "first", split_axis=2, concat_axis=0, tiled=True),
    )
    strip = jnp.einsum(
        "kid,kjd->ijd",
        lax.all_gather(left_lines, "second", axis=1, tiled=True),
        right_lines,
        preferred_element_type=jnp.float32,
    )
    strip = (strip * count ** (-0.5)).astype(jnp.bfloat16)
    mixed = lax.all_to_all(strip, "first", split_axis=0, concat_axis=2, tiled=True)
    scaled = norm_channels(mixed.astype(jnp.float32), mid_gain).astype(jnp.bfloat16)
    scaled = lax.optimization_barrier(scaled)
    gate = jax.nn.sigmoid(
        jnp.einsum("ijc,cd->ijd", ready, out_gate, preferred_element_type=jnp.float32)
    )
    return (
        jnp.einsum("ijd,dc->ijc", scaled, out_weight, preferred_element_type=jnp.float32) * gate
    ).astype(jnp.bfloat16)


def solution(mesh):
    in_specs = (P("first", "second", None), P(), P(), P(), P(), P(), P())
    out_specs = P("first", "second", None)
    planes, lines = mesh.shape["first"] // 2, mesh.shape["second"]
    if planes == lines == 4:
        body = functools.partial(triangle, planes, lines)
    else:
        body = shards
    return jax.shard_map(body, mesh=mesh, in_specs=in_specs, out_specs=out_specs, check_vma=False)
```
